32 devices in a mesh: blk: 8 (over z, y), sub: 4 (over x, core).
Axes of the slice: x: 2, y: 2, z: 4, core: 2. Of those that a mesh axis runs over, the one named last changes fastest.
Arguments:
- solution: float32 [5, 8, 32, 512], P(None, 'blk', 'sub'), may hold values from -6 to 6
- right_side: float32 [5, 8, 32, 512], P(None, 'blk', 'sub'), may hold values from -6 to 6
- couple: float32 [3, 7, 5, 5], replicated, may hold values from -0.06 to 1.1, as said below
- partner: int32 [8], replicated, may hold values from 0 to 7, each once
- orient: int32 [8], replicated, may hold values from 0 to 3
- owner_one: int32 [8], replicated, may hold values from 0 to 7, each once
- owner_two: int32 [8], replicated, may hold values from 0 to 7, each once
Outputs:
- corrected: float32 [5, 8, 32, 512], P(None, 'blk', 'sub')
- coarse_one: float32 [5, 8, 16, 128], P(None, 'blk', 'sub')
- coarse_two: float32 [5, 8, 8, 32], P(None, 'blk', 'sub')
- norms: float32 [3], replicated
The draws below stay inside these ranges and needn't reach their ends.
Inputs may be any that keep to these rules, and one draw needn't show every extreme that they name: `couple`: each level's centre matrix has diagonal entries of 0.9 to 1.1 and off-diagonal entries of magnitude 0.06 or less; every coupling's entries lie in the stated range. `partner`: A permutation of the 8 blocks. `owner_one`: A permutation of the 8 blocks. `owner_two`: A permutation of the 8 blocks.
All inputs are finite; a program needn't handle non-finite values.
Results may differ from the reference program's by a relative error of at most 0.00025.
Values sent between devices are 32-bit elements; how exact they have to be, the bound alone decides.
A program may use at most 64 MiB of HBM per device.

```python
import jax
import jax.numpy as jnp
from jax import lax

NV = 5
BI = 32
BJ = 16
SWEEPS_FINE = 2
SWEEPS_MID = 2
SWEEPS_COARSE = 4
NB = 8
K0 = 32
PL0 = 512


def draw_couple(key, part):
    jitter = jax.random.uniform(key, (3, 7, NV, NV), jnp.float32, -1.0, 1.0)
    diagonal = jnp.array([1.0, 0.015, 0.015, 0.015, 0.015, 0.8, 0.04], jnp.float32)
    spread = jnp.array([0.06, 0.006, 0.006, 0.006, 0.006, 0.05, 0.012], jnp.float32)
    identity = jnp.eye(NV, dtype=jnp.float32)
    leading = diagonal[None, :, None, None] * (1.0 + 0.1 * jitter)
    lateral = spread[None, :, None, None] * jitter
    return identity * leading + (1.0 - identity) * lateral


def set_ends(values, key, least, largest):
    place = [jax.random.randint(jax.random.fold_in(key, axis), (), 0, length) for axis, length in enumerate(values.shape)]
    widest = values.shape.index(max(values.shape))
    next_to = place[:widest] + [(place[widest] + 1) % values.shape[widest]] + place[widest + 1:]
    return values.at[tuple(place)].set(least).at[tuple(next_to)].set(largest)


def levels(stream_key, dims, pieces, smallest, top_value):
    def one(dim, shards_of):
        steps = jax.random.uniform(jax.random.fold_in(jax.random.fold_in(stream_key, 6), dim), (shards_of,), jnp.float32, smallest / len(pieces), top_value / len(pieces))
        return jnp.repeat(jnp.exp(steps), dims[dim] // shards_of).reshape((-1,) + (1,) * (len(dims) - dim - 1))

    gain = one(*pieces[0])
    for cut in pieces[1:]:
        gain = gain * one(*cut)
    return gain


def noise(own_key, dims, deviation, bound, split=(), kind=jnp.bfloat16):
    factor_of = levels(own_key, dims, split, -0.22, 0.18) if split else 1.0
    result = jax.random.normal(own_key, dims, jnp.float32) * deviation * factor_of
    return jnp.minimum(jnp.maximum(result, -bound), bound).astype(kind)


def setup_inputs(seed: int = 0) -> dict:
    streams_of = jax.random.split(jax.random.key(seed), 8)
    return {
        "solution": noise(streams_of[0], (NV, NB, K0, PL0), 1.0, 6.0, ((1, 8), (2, 4)), jnp.float32),
        "right_side": noise(streams_of[1], (NV, NB, K0, PL0), 1.0, 6.0, ((1, 8), (2, 4)), jnp.float32),
        "couple": draw_couple(jax.random.fold_in(streams_of[7], 71), 0),
        "partner": jax.random.permutation(streams_of[3], NB).astype(jnp.int32),
        "orient": set_ends(jax.random.randint(streams_of[4], (NB,), 0, 4), jax.random.fold_in(streams_of[4], 1), 0, 3).astype(jnp.int32),
        "owner_one": jax.random.permutation(streams_of[5], NB).astype(jnp.int32),
        "owner_two": jax.random.permutation(streams_of[6], NB).astype(jnp.int32),
    }


PRECISE = lax.Precision.HIGHEST

def apply_matrix(matrix, values):
    return jnp.einsum('ab,b...->a...', matrix, values, precision=PRECISE)

def invert(matrix):
    identity = jnp.eye(matrix.shape[0], dtype=matrix.dtype)
    approx = identity
    for repeat in range(6):
        approx = jnp.dot(approx, 2.0 * identity - jnp.dot(matrix, approx, precision=PRECISE), precision=PRECISE)
    return approx

def level_matrices(couple, level):
    center = couple[level, 0]
    inverse = invert(center)
    lateral = (couple[level, 1], couple[level, 2], couple[level, 3], couple[level, 4])
    below_coupling = couple[level, 5]
    above_coupling = couple[level, 6]
    forward = jnp.dot(inverse, below_coupling, precision=PRECISE)
    backward = jnp.dot(inverse, above_coupling, precision=PRECISE)
    return (center, inverse, lateral, below_coupling, above_coupling, forward, backward)

def in_plane(lateral, values, rows_i, rows_j):
    shaped = values.reshape(values.shape[:-1] + (rows_i, rows_j))
    pad_widths = [(0, 0)] * (shaped.ndim - 2) + [(1, 1), (1, 1)]
    padded = jnp.pad(shaped, pad_widths)
    summed = apply_matrix(lateral[0], padded[..., :-2, 1:-1]) + apply_matrix(lateral[1], padded[..., 2:, 1:-1])
    summed = summed + apply_matrix(lateral[2], padded[..., 1:-1, :-2]) + apply_matrix(lateral[3], padded[..., 1:-1, 2:])
    return summed.reshape(values.shape)

def flip_planes(planes, codes, rows_i, rows_j):
    shaped = planes.reshape(planes.shape[:-1] + (rows_i, rows_j))
    first_flip = jnp.where((codes % 2 == 1)[None, :, None, None], shaped[..., ::-1, :], shaped)
    both_flips = jnp.where((codes // 2 == 1)[None, :, None, None], first_flip[..., ::-1], first_flip)
    return both_flips.reshape(planes.shape)

def inverse_map(mapping):
    indices = jnp.arange(mapping.shape[0], dtype=jnp.int32)
    return lax.optimization_barrier(jnp.sum(jnp.where(mapping[None, :] == indices[:, None], indices[None, :], 0), axis=1)).astype(jnp.int32)

def interfaces(iterate, partner, orient, rows_i, rows_j):
    down_map = inverse_map(partner)
    below = flip_planes(iterate[:, down_map, -1, :], orient[down_map], rows_i, rows_j)
    above = flip_planes(iterate[:, partner, 0, :], orient, rows_i, rows_j)
    return (below, above)

def residual_of(iterate, source_term, matrices, partner, orient, rows_i, rows_j):
    center, inverse, lateral, below_coupling, above_coupling, forward, backward = matrices
    below, above = interfaces(iterate, partner, orient, rows_i, rows_j)
    lower = jnp.concatenate([below[:, :, None], iterate[:, :, :-1]], axis=2)
    upper = jnp.concatenate([iterate[:, :, 1:], above[:, :, None]], axis=2)
    image = apply_matrix(center, iterate) - in_plane(lateral, iterate, rows_i, rows_j)
    image = image - apply_matrix(below_coupling, lower) - apply_matrix(above_coupling, upper)
    return source_term - image

def sweep_of(iterate, source_term, matrices, partner, orient, rows_i, rows_j):
    center, inverse, lateral, below_coupling, above_coupling, forward, backward = matrices
    below, above = interfaces(iterate, partner, orient, rows_i, rows_j)
    planes_count = iterate.shape[2]
    upper = jnp.concatenate([iterate[:, :, 1:], above[:, :, None]], axis=2)
    source = source_term + in_plane(lateral, iterate, rows_i, rows_j) + apply_matrix(above_coupling, upper)
    scaled = apply_matrix(inverse, source)
    previous = below
    stacked = []
    for position in range(planes_count):
        previous = scaled[:, :, position] + apply_matrix(forward, previous)
        stacked.append(previous)
    forward_field = jnp.stack(stacked, axis=2)
    lower = jnp.concatenate([below[:, :, None], forward_field[:, :, :-1]], axis=2)
    source_back = source_term + in_plane(lateral, forward_field, rows_i, rows_j) + apply_matrix(below_coupling, lower)
    scaled_back = apply_matrix(inverse, source_back)
    following = above
    stacked_back = []
    for position in range(planes_count - 1, -1, -1):
        following = scaled_back[:, :, position] + apply_matrix(backward, following)
        stacked_back.append(following)
    return jnp.stack(stacked_back[::-1], axis=2)

def restrict(values, rows_i, rows_j):
    shape_in = values.shape
    shaped = values.reshape(shape_in[0], shape_in[1], shape_in[2] // 2, 2, rows_i // 2, 2, rows_j // 2, 2)
    averaged = lax.optimization_barrier(jnp.mean(shaped, axis=(3, 5, 7)))
    return averaged.reshape(shape_in[0], shape_in[1], shape_in[2] // 2, shape_in[3] // 4)

def prolong(values, rows_i, rows_j):
    shape_in = values.shape
    shaped = values.reshape(shape_in[0], shape_in[1], shape_in[2], 1, rows_i, 1, rows_j, 1)
    spread_out = jnp.broadcast_to(shaped, (shape_in[0], shape_in[1], shape_in[2], 2, rows_i, 2, rows_j, 2))
    return spread_out.reshape(shape_in[0], shape_in[1], shape_in[2] * 2, shape_in[3] * 4)

def reference(solution, right_side, couple, partner, orient, owner_one, owner_two):
    matrices = [level_matrices(couple, level) for level in range(3)]
    iterate = solution
    for repeat in range(SWEEPS_FINE):
        iterate = sweep_of(iterate, right_side, matrices[0], partner, orient, BI, BJ)
    residual_zero = residual_of(iterate, right_side, matrices[0], partner, orient, BI, BJ)
    source_one = restrict(residual_zero, BI, BJ)
    iterate_one = jnp.zeros_like(source_one)
    for repeat in range(SWEEPS_MID):
        iterate_one = sweep_of(iterate_one, source_one, matrices[1], partner, orient, BI // 2, BJ // 2)
    residual_one = residual_of(iterate_one, source_one, matrices[1], partner, orient, BI // 2, BJ // 2)
    source_two = restrict(residual_one, BI // 2, BJ // 2)
    iterate_two = jnp.zeros_like(source_two)
    for repeat in range(SWEEPS_COARSE):
        iterate_two = sweep_of(iterate_two, source_two, matrices[2], partner, orient, BI // 4, BJ // 4)
    residual_two = residual_of(iterate_two, source_two, matrices[2], partner, orient, BI // 4, BJ // 4)
    norms = jnp.stack([jnp.sqrt(jnp.mean(residual_zero * residual_zero)), jnp.sqrt(jnp.mean(residual_one * residual_one)), jnp.sqrt(jnp.mean(residual_two * residual_two))])
    iterate_one = iterate_one + prolong(iterate_two, BI // 4, BJ // 4)
    corrected = iterate + prolong(iterate_one, BI // 2, BJ // 2)
    coarse_one = iterate_one[:, inverse_map(owner_one)]
    coarse_two = iterate_two[:, inverse_map(owner_two)]
    return (corrected, coarse_one, coarse_two, norms)
```

```python
import functools

import jax
import jax.numpy as jnp
from jax import lax
from jax.experimental import pallas as pl
from jax.experimental.pallas import tpu as pltpu
from jax.sharding import PartitionSpec as P

BI = 32
BJ = 16
SWEEPS_FINE = 2
SWEEPS_MID = 2
SWEEPS_COARSE = 4
LANES = 128
SUBLANES = 8
NV = 5
PRECISE = lax.Precision.HIGHEST
MESH = pl.DeviceIdType.MESH

RAW = 0
INV, IM, IP, JM, JP, FWD, BWD = 7, 8, 9, 10, 11, 12, 13
F2, F4, F8, FP, B2, B4, B8, BP = 14, 15, 16, 17, 18, 19, 20, 21


def product(left, right):
    total = left[0][None] * right[:, 0][:, None]
    for b in range(1, NV):
        total = total + left[b][None] * right[:, b][:, None]
    return total


def kernel(
    sizes, solution, right_side, couple, partner, orient, owner_one, owner_two,
    corrected, out_one, out_two, norms,
    coef, coef_one, coef_two, cg, sf, yf, tf, zf, enter, plane_below, plane_above,
    xsend, xrecv_a, xrecv_b, xrecv_c, up_recv, low_recv, prefix, gathered, rsum,
    down,
    field_f, field_c, field_p, field_v, field_y,
    two_f, two_c, two_p, two_v, two_y, spread,
    xs_sem, xr_sem, hs_sem, hr_sem, ps_sem, pr_sem, gs_sem, gr_sem, es_sem, er_sem,
):
    blocks, subs = sizes
    me = lax.axis_index("blk")
    sub = lax.axis_index("sub")
    last = subs - 1
    is_low = sub == 0
    is_high = sub == last
    rows = solution.shape[1]
    planes = SUBLANES
    xrecv = (xrecv_a, xrecv_b, xrecv_c)

    def edge_copy(t, b):
        return pltpu.make_async_remote_copy(
            src_ref=xsend.at[t], dst_ref=xrecv[t].at[me], send_sem=xs_sem.at[t, b],
            recv_sem=xr_sem.at[t, me], device_id=(b, last - sub), device_id_type=MESH)

    def edge_wait(t, b):
        pltpu.make_async_remote_copy(
            src_ref=xsend.at[t], dst_ref=xrecv[t].at[b], send_sem=xs_sem.at[t, b],
            recv_sem=xr_sem.at[t, b], device_id=(b, last - sub), device_id_type=MESH).wait_recv()

    def send_edge(t, ref):
        @pl.when(is_low)
        def _():
            xsend[t] = ref[:, :, 0:1, :]

        @pl.when(is_high)
        def _():
            xsend[t] = ref[:, :, planes - 1:planes, :]

        @pl.when(is_low | is_high)
        def _():
            @pl.loop(0, blocks)
            def _(b):
                edge_copy(t, b).start()

    lane = lax.broadcasted_iota(jnp.int32, (1, LANES), 1)

    def lane_xor(x, bit):
        axis = x.ndim - 1
        mask = (lane & bit) != 0
        return jnp.where(mask, pltpu.roll(x, bit, axis), pltpu.roll(x, LANES - bit, axis))

    def receive_edge(t):
        @pl.when(is_low | is_high)
        def _():
            @pl.loop(0, blocks)
            def _(b):
                edge_wait(t, b)

        def oriented(source, code):
            got = xrecv[t][source]
            swapped = jnp.concatenate([got[:, r:r + 1] for r in range(rows - 1, -1, -1)], axis=1)
            for bit in (16, 32, 64):
                swapped = lane_xor(swapped, bit)
            got = jnp.where(code % 2 == 1, swapped, got)
            swapped = got
            for bit in (1, 2, 4, 8):
                swapped = lane_xor(swapped, bit)
            return jnp.where(code // 2 == 1, swapped, got)

        @pl.when(is_low)
        def _():
            source = down[me]
            plane_below[...] = oriented(source, orient[source])

        @pl.when(is_high)
        def _():
            plane_above[...] = oriented(partner[me], orient[me])

    def halo_copy(which, src, dst, target):
        return pltpu.make_async_remote_copy(
            src_ref=src, dst_ref=dst, send_sem=hs_sem.at[which], recv_sem=hr_sem.at[which],
            device_id=(me, target), device_id_type=MESH)

    def prefix_copy(n, source, target):
        return pltpu.make_async_remote_copy(
            src_ref=prefix.at[n, source], dst_ref=prefix.at[n, source], send_sem=ps_sem.at[n, target],
            recv_sem=pr_sem.at[n, source], device_id=(me, target), device_id_type=MESH)

    here = me * subs + sub

    @pl.loop(1, blocks * subs)
    def _(step):
        there = (here + step) % (blocks * subs)
        pl.semaphore_signal(pltpu.get_barrier_semaphore(), inc=1,
                            device_id=(there // subs, there % subs), device_id_type=MESH)

    def found(mapping, value):
        return lax.fori_loop(0, blocks, lambda n, best: jnp.where(mapping[n] == value, n, best), 0)

    @pl.loop(0, blocks)
    def _(n):
        down[n] = found(partner, n)

    held = (found(owner_one, me), found(owner_two, me))

    def splat(level, matrix):
        return jnp.stack([
            jnp.stack([jnp.full((SUBLANES, LANES), couple[a, b, level, matrix], jnp.float32) for a in range(NV)])
            for b in range(NV)
        ])

    identity = jnp.stack([
        jnp.stack([jnp.full((SUBLANES, LANES), 1.0 if a == b else 0.0, jnp.float32) for a in range(NV)])
        for b in range(NV)
    ])

    def prepare(level, store):
        for matrix in range(7):
            store[RAW + matrix] = splat(level, matrix)
        store[INV] = identity

        @pl.loop(0, 6)
        def _(repeat):
            approx = store[INV]
            store[INV] = product(approx, 2.0 * identity - product(store[RAW], approx))

        @pl.loop(0, 6)
        def _(matrix):
            store[IM + matrix] = product(store[INV], store[RAW + 1 + matrix])

    prepare(0, coef)
    place = lax.broadcasted_iota(jnp.int32, (SUBLANES, LANES), 0)

    def powers(base, second, count):
        coef[second] = product(coef[base], coef[base])
        coef[second + 1] = product(coef[second], coef[second])
        coef[second + 2] = product(coef[second + 1], coef[second + 1])
        run = jnp.where((count & 1) != 0, coef[base], identity)
        for bit, index in ((2, second), (4, second + 1), (8, second + 2)):
            run = product(jnp.where((count & bit) != 0, coef[index], identity), run)
        coef[second + 3] = run

    powers(FWD, F2, place + 1)
    powers(BWD, B2, planes - place)

    def apply(index, values, height=SUBLANES):
        total = None
        for b in range(NV):
            term = coef[index, b][:, None, :height] * values[b][None]
            total = term if total is None else total + term
        return total

    in_low = lane < BJ
    in_high = lane >= LANES - BJ
    j_first = (lane & (BJ - 1)) == 0
    j_final = (lane & (BJ - 1)) == BJ - 1

    def lateral(values, base):
        zero = jnp.zeros_like(values[:, :1])
        turned = pltpu.roll(values, BJ, 3)
        total = apply(base, jnp.where(in_low, jnp.concatenate([zero, turned[:, :-1]], axis=1), turned))
        turned = pltpu.roll(values, LANES - BJ, 3)
        total = total + apply(base + 1, jnp.where(in_high, jnp.concatenate([turned[:, 1:], zero], axis=1), turned))
        total = total + apply(base + 2, jnp.where(j_first, 0.0, pltpu.roll(values, 1, 3)))
        return total + apply(base + 3, jnp.where(j_final, 0.0, pltpu.roll(values, LANES - 1, 3)))

    def moved_up(values, by):
        return pltpu.roll(values, by, 2)

    def scan(values, first, second, reverse):
        for by, index in ((1, first), (2, second), (4, second + 1)):
            if reverse:
                shifted = jnp.where(place < planes - by, pltpu.roll(values, planes - by, 2), 0.0)
            else:
                shifted = jnp.where(place >= by, pltpu.roll(values, by, 2), 0.0)
            values = values + apply(index, shifted)
        return values

    def complete(n, ref, boundary, reverse, index_all, index_block):
        starts = is_high if reverse else is_low

        @pl.when(starts)
        def _():
            ref[...] = ref[...] + apply(index_all, boundary[...])

        prefix[n, sub] = ref[:, :, 0:1, :] if reverse else ref[:, :, planes - 1:planes, :]
        for target in range(subs):
            @pl.when((target < sub) if reverse else (target > sub))
            def _():
                prefix_copy(n, sub, target).start()

        @pl.when(jnp.logical_not(starts))
        def _():
            enter[...] = jnp.zeros_like(enter)
            order = range(last, 0, -1) if reverse else range(last)
            for source in order:
                @pl.when((source > sub) if reverse else (source < sub))
                def _():
                    prefix_copy(n, source, sub).wait_recv()
                    enter[...] = prefix[n, source] + apply(index_block, enter[...], 1)
            ref[...] = ref[...] + apply(index_all, enter[...])

    up_recv[1] = solution[:, :, 0:1, :]
    cg[...] = apply(INV, right_side[...])
    sf[...] = cg[...] + lateral(solution[...], IM)
    pl.semaphore_wait(pltpu.get_barrier_semaphore(), blocks * subs - 1)
    send_edge(0, solution)

    @pl.when(jnp.logical_not(is_low))
    def _():
        halo_copy(0, up_recv.at[1], up_recv.at[0], sub - 1).start()
    for t in range(SWEEPS_FINE):
        if t > 0:
            sf[...] = cg[...] + lateral(zf[...], IM) + (zf[...] - tf[...])
        receive_edge(t)
        if t == 0:
            @pl.when(is_high)
            def _():
                up_recv[0] = plane_above[...]

            @pl.when(jnp.logical_not(is_high))
            def _():
                halo_copy(0, up_recv.at[1], up_recv.at[0], sub).wait_recv()

            upper = jnp.where(place == planes - 1, up_recv[0], pltpu.roll(solution[...], planes - 1, 2))
            sf[...] = sf[...] + apply(BWD, upper)
        else:
            @pl.when(is_high)
            def _():
                fresh = apply(BWD, plane_above[...], 1)
                old = zf[:, :, planes - 1:planes, :] - tf[:, :, planes - 1:planes, :]
                sf[:, :, planes - 1:planes, :] = sf[:, :, planes - 1:planes, :] + (fresh - old)

        yf[...] = scan(sf[...], FWD, F2, False)
        complete(2 * t, yf, plane_below, False, FP, F8)
        tf[...] = cg[...] + lateral(yf[...], IM) + (yf[...] - sf[...])
        zf[...] = scan(tf[...], BWD, B2, True)
        complete(2 * t + 1, zf, plane_above, True, BP, B8)
        send_edge(t + 1, zf)
        if t == 0:
            prepare(1, coef_one)
            prepare(2, coef_two)

    up_recv[2] = zf[:, :, 0:1, :]
    low_recv[1] = zf[:, :, planes - 1:planes, :]

    @pl.when(jnp.logical_not(is_low))
    def _():
        halo_copy(1, up_recv.at[2], up_recv.at[3], sub - 1).start()

    @pl.when(jnp.logical_not(is_high))
    def _():
        halo_copy(2, low_recv.at[1], low_recv.at[0], sub + 1).start()

    partial = right_side[...] - (apply(RAW, zf[...]) - lateral(zf[...], RAW + 1))
    height = rows * LANES
    r_row = lax.broadcasted_iota(jnp.int32, (height, LANES), 0)
    r_col = lax.broadcasted_iota(jnp.int32, (height, LANES), 1)
    half = BJ // 2
    share = (((r_row >> 5) * half) + ((r_row & (BJ - 1)) >> 1) == r_col).astype(jnp.float32)

    receive_edge(SWEEPS_FINE)

    @pl.when(is_low)
    def _():
        low_recv[0] = plane_below[...]

    @pl.when(is_high)
    def _():
        up_recv[3] = plane_above[...]

    @pl.when(jnp.logical_not(is_high))
    def _():
        halo_copy(1, up_recv.at[2], up_recv.at[3], sub).wait_recv()

    @pl.when(jnp.logical_not(is_low))
    def _():
        halo_copy(2, low_recv.at[1], low_recv.at[0], sub).wait_recv()

    lower = jnp.where(place == 0, low_recv[0], pltpu.roll(zf[...], 1, 2))
    upper = jnp.where(place == planes - 1, up_recv[3], pltpu.roll(zf[...], planes - 1, 2))
    residual = partial + apply(RAW + 5, lower) + apply(RAW + 6, upper)
    squares = jnp.sum((residual * residual).reshape(NV * rows, SUBLANES, LANES), axis=0)

    reduced = None
    for r in range(rows):
        term = jnp.dot(residual[:, r].reshape(NV * SUBLANES, LANES), share[r * LANES:(r + 1) * LANES],
                       precision=PRECISE, preferred_element_type=jnp.float32)
        reduced = term if reduced is None else reduced + term
    count = NV * planes // 2
    rsum[...] = reduced * 0.125
    gathered[sub, me, 0:count, :] = rsum[pl.ds(0, count, stride=2), :] + rsum[pl.ds(1, count, stride=2), :]
    gathered[sub, me, count:count + 1, :] = jnp.sum(squares, axis=0, keepdims=True)
    filler = gathered.shape[2] - count - 1
    gathered[sub, me, count + 1:, :] = jnp.zeros((filler, LANES), jnp.float32)

    def spread_copy(source, target):
        return pltpu.make_async_remote_copy(
            src_ref=gathered.at[sub, source], dst_ref=gathered.at[sub, source], send_sem=gs_sem.at[target],
            recv_sem=gr_sem.at[source], device_id=(target, sub), device_id_type=MESH)

    @pl.loop(1, blocks)
    def _(step):
        spread_copy(me, (me + step) % blocks).start()

    def across_copy(source, block, target):
        return pltpu.make_async_remote_copy(
            src_ref=gathered.at[source, block], dst_ref=gathered.at[source, block],
            send_sem=es_sem.at[target, block], recv_sem=er_sem.at[source, block],
            device_id=(me, target), device_id_type=MESH)

    for step in range(1, subs):
        across_copy(sub, me, (sub + step) % subs).start()

    @pl.loop(1, blocks)
    def _(step):
        source = (me + step) % blocks
        spread_copy(source, source).wait_recv()
        for turn in range(1, subs):
            across_copy(sub, source, (sub + turn) % subs).start()

    @pl.loop(0, blocks)
    def _(block):
        for turn in range(1, subs):
            source = (sub + turn) % subs
            across_copy(source, block, source).wait_recv()

    local = planes // 2
    total = jnp.zeros((1, LANES), jnp.float32)
    for s in range(subs):
        for a in range(NV):
            for k in range(local):
                field_f[a, s * local + k] = gathered[s, :, a * local + k, :]
        total = total + jnp.sum(gathered[s, :, count, :], axis=0, keepdims=True)

    def root_mean(value, entries):
        return jnp.sqrt(jnp.sum(value, axis=1, keepdims=True) / jnp.float32(entries))

    size = NV * blocks * subs * planes * rows * LANES
    norms[0:1, :] = jnp.broadcast_to(root_mean(total, size), (1, LANES))

    def level(store, cells, width, g, c, p, v, y, sweeps):
        depth = g.shape[1]
        inside = lane < cells
        mask_im = (lane >= width) & inside
        mask_ip = lane < cells - width
        mask_jm = ((lane & (width - 1)) != 0) & inside
        mask_jp = ((lane & (width - 1)) != width - 1) & inside
        bits = [1 << n for n in range(cells.bit_length() - 1)]
        bits_j = [n for n in bits if n < width]
        bits_i = [n for n in bits if n >= width]
        chunk = max(1, 4 * SUBLANES // blocks)

        def use(index, values):
            cut = values.reshape(NV, -1, SUBLANES, LANES)
            terms = [store[index, b][:, None] * cut[b][None] for b in range(NV)]
            out = (terms[0] + terms[1]) + (terms[2] + terms[3]) + terms[4]
            return out.reshape(values.shape)

        def sides(values, base):
            axis = values.ndim - 1
            out = use(base, jnp.where(mask_im, pltpu.roll(values, width, axis), 0.0))
            out = out + use(base + 1, jnp.where(mask_ip, pltpu.roll(values, LANES - width, axis), 0.0))
            out = out + use(base + 2, jnp.where(mask_jm, pltpu.roll(values, 1, axis), 0.0))
            return out + use(base + 3, jnp.where(mask_jp, pltpu.roll(values, LANES - 1, axis), 0.0))

        def flipped(values, odd, high):
            swapped = values
            for bit in bits_i:
                swapped = lane_xor(swapped, bit)
            values = jnp.where(odd, swapped, values)
            swapped = values
            for bit in bits_j:
                swapped = lane_xor(swapped, bit)
            return jnp.where(high, swapped, values)

        slot = lax.broadcasted_iota(jnp.int32, (blocks, 1), 0)

        def codes(source):
            out = jnp.zeros((blocks, 1), jnp.int32)
            for n in range(blocks):
                out = jnp.where(slot == n, source(n), out)
            return out

        code_below = codes(lambda n: orient[down[n]])
        code_above = codes(lambda n: orient[n])

        def interfaces():
            below = jnp.concatenate([v[:, depth - 1, pl.ds(down[n], 1), :] for n in range(blocks)], axis=1)
            above = jnp.concatenate([v[:, 0, pl.ds(partner[n], 1), :] for n in range(blocks)], axis=1)
            below = flipped(below, (code_below & 1) != 0, code_below >= 2)
            above = flipped(above, (code_above & 1) != 0, code_above >= 2)
            return below, above

        @pl.loop(0, depth // chunk)
        def _(step):
            at = pl.ds(step * chunk, chunk)
            c[:, at] = use(INV, g[:, at])

        nothing = jnp.zeros((NV, blocks, LANES), jnp.float32)
        below, above = nothing, nothing
        for n in range(sweeps):
            if n > 0:
                below, above = interfaces()
                p[:, depth - 1] = use(BWD, above)

            def forward(step, previous):
                at = pl.ds(step * chunk, chunk)
                s = c[:, at]
                if n > 0:
                    s = s + sides(v[:, at], IM) + p[:, at]
                made = []
                for u in range(chunk):
                    behind = use(FWD, previous)
                    previous = s[:, u] + behind
                    made.append((previous, behind))
                for u, (now, behind) in enumerate(made):
                    y[:, step * chunk + u] = now
                    p[:, step * chunk + u] = behind
                return previous

            lax.fori_loop(0, depth // chunk, forward, below)

            def backward(step, following):
                start = depth - chunk - step * chunk
                at = pl.ds(start, chunk)
                t = c[:, at] + sides(y[:, at], IM) + p[:, at]
                made = []
                for u in range(chunk - 1, -1, -1):
                    ahead = use(BWD, following)
                    following = t[:, u] + ahead
                    made.append((u, following, ahead))
                for u, now, ahead in made:
                    v[:, start + u] = now
                    p[:, start + u] = ahead
                return following

            lax.fori_loop(0, depth // chunk, backward, above)
        below, above = interfaces()
        y[:, 0] = below

        @pl.loop(1, depth)
        def _(k):
            y[:, k] = v[:, k - 1]

        p[:, depth - 1] = above

        @pl.loop(0, depth - 1)
        def _(k):
            p[:, k] = v[:, k + 1]

        def remain(step, squares):
            at = pl.ds(step * chunk, chunk)
            now = v[:, at]
            image = use(RAW, now) - sides(now, RAW + 1) - use(RAW + 5, y[:, at]) - use(RAW + 6, p[:, at])
            out = g[:, at] - image
            c[:, at] = out
            return squares + jnp.sum(out * out, axis=1)

        squares = lax.fori_loop(0, depth // chunk, remain, nothing)
        return jnp.sum(squares.reshape(NV * blocks, LANES), axis=0, keepdims=True)

    depth_one = field_f.shape[1]
    cells_one = rows * LANES // 4
    total = level(coef_one, cells_one, BJ // 2, field_f, field_c, field_p, field_v, field_y, SWEEPS_MID)
    norms[1:2, :] = jnp.broadcast_to(root_mean(total, size // 8), (1, LANES))

    s_row = lax.broadcasted_iota(jnp.int32, (LANES, LANES), 0)
    s_col = lax.broadcasted_iota(jnp.int32, (LANES, LANES), 1)
    fold = (((s_row >> 4) * (BJ // 4)) + ((s_row & (BJ // 2 - 1)) >> 1) == s_col).astype(jnp.float32)
    depth_two = depth_one // 2

    @pl.loop(0, depth_two)
    def _(k):
        pair = (field_c[:, 2 * k] + field_c[:, 2 * k + 1]) * 0.125
        two_f[:, k] = jnp.dot(pair.reshape(NV * blocks, LANES), fold, precision=PRECISE,
                              preferred_element_type=jnp.float32).reshape(NV, blocks, LANES)

    total = level(coef_two, cells_one // 4, BJ // 4, two_f, two_c, two_p, two_v, two_y, SWEEPS_COARSE)
    norms[2:3, :] = jnp.broadcast_to(root_mean(total, size // 64), (1, LANES))

    unfold = (((s_col >> 4) * (BJ // 4)) + ((s_col & (BJ // 2 - 1)) >> 1) == s_row).astype(jnp.float32)

    @pl.loop(0, depth_two)
    def _(k):
        grown = jnp.dot(two_v[:, k].reshape(NV * blocks, LANES), unfold, precision=PRECISE,
                        preferred_element_type=jnp.float32).reshape(NV, blocks, LANES)
        field_v[:, 2 * k] = field_v[:, 2 * k] + grown
        field_v[:, 2 * k + 1] = field_v[:, 2 * k + 1] + grown

    for a in range(NV):
        for k in range(local):
            row = field_v[a, sub * local + k, pl.ds(me, 1), :]
            spread[pl.ds(a * planes + 2 * k, 2), :] = jnp.broadcast_to(row, (2, LANES))
            out_one[a, pl.ds(k, 1), :] = field_v[a, sub * local + k, pl.ds(held[0], 1), :]
        for k in range(local // 2):
            out_two[a, pl.ds(k, 1), :] = two_v[a, sub * (local // 2) + k, pl.ds(held[1], 1), :]

    c_row = lax.broadcasted_iota(jnp.int32, (LANES, LANES), 0)
    c_col = lax.broadcasted_iota(jnp.int32, (LANES, LANES), 1)
    for r in range(rows):
        grow = ((((c_col + r * LANES) >> 5) * half) + ((c_col & (BJ - 1)) >> 1) == c_row).astype(jnp.float32)
        grown = jnp.dot(spread[...], grow, precision=PRECISE, preferred_element_type=jnp.float32)
        corrected[:, r] = zf[:, r] + grown.reshape(NV, SUBLANES, LANES)

    for t in range(SWEEPS_FINE + 1):
        @pl.when(is_low | is_high)
        def _():
            @pl.loop(0, blocks)
            def _(b):
                edge_copy(t, b).wait_send()

    @pl.when(jnp.logical_not(is_low))
    def _():
        halo_copy(0, up_recv.at[1], up_recv.at[0], sub - 1).wait_send()
        halo_copy(1, up_recv.at[2], up_recv.at[3], sub - 1).wait_send()

    @pl.when(jnp.logical_not(is_high))
    def _():
        halo_copy(2, low_recv.at[1], low_recv.at[0], sub + 1).wait_send()

    for n in range(2 * SWEEPS_FINE):
        for target in range(subs):
            @pl.when((target < sub) if n % 2 else (target > sub))
            def _():
                prefix_copy(n, sub, target).wait_send()

    @pl.loop(1, blocks)
    def _(step):
        spread_copy(me, (me + step) % blocks).wait_send()

    @pl.loop(0, blocks)
    def _(block):
        for turn in range(1, subs):
            across_copy(sub, block, (sub + turn) % subs).wait_send()


def finish(corrected, one, two, norms, out, out_one, out_two, out_norms):
    for r in range(corrected.shape[1]):
        out[:, 0, :, r * LANES:(r + 1) * LANES] = corrected[:, r]
    out_one[:, 0] = one[...]
    out_two[:, 0] = two[:, :, :out_two.shape[3]]
    for n in range(3):
        out_norms[n] = jnp.max(norms[n:n + 1, :])


def shards(solution, right_side, couple, partner, orient, owner_one, owner_two):
    blocks = lax.axis_size("blk")
    subs = lax.axis_size("sub")
    planes, cells = solution.shape[2:]
    rows = cells // LANES
    tall = planes * subs

    def tiled(x):
        return x.reshape(NV, planes, rows, LANES).transpose(0, 2, 1, 3)

    vmem = pl.BlockSpec(memory_space=pltpu.VMEM)
    smem = pl.BlockSpec(memory_space=pltpu.SMEM)
    f32 = jnp.float32
    fine = pltpu.VMEM((NV, rows, planes, LANES), f32)
    plane = (NV, rows, 1, LANES)
    mid = pltpu.VMEM((NV, tall // 2, blocks, LANES), f32)
    low = pltpu.VMEM((NV, tall // 4, blocks, LANES), f32)
    matrix = (NV, NV, SUBLANES, LANES)
    payload = NV * planes // 2 + 4
    dma = pltpu.SemaphoreType.DMA
    edges = SWEEPS_FINE + 1
    corrected, one, two, norms = pl.pallas_call(
        functools.partial(kernel, (blocks, subs)),
        name="vcycle",
        out_shape=(
            pltpu.VMEM((NV, rows, planes, LANES), f32),
            pltpu.VMEM((NV, planes // 2, LANES), f32),
            pltpu.VMEM((NV, planes // 4, LANES), f32),
            pltpu.VMEM((3, LANES), f32),
        ),
        in_specs=[vmem, vmem, smem, smem, smem, smem, smem],
        out_specs=(vmem, vmem, vmem, vmem),
        scratch_shapes=[
            pltpu.VMEM((22,) + matrix, f32), pltpu.VMEM((14,) + matrix, f32), pltpu.VMEM((14,) + matrix, f32),
            fine, fine, fine, fine, fine,
            pltpu.VMEM(plane, f32), pltpu.VMEM(plane, f32), pltpu.VMEM(plane, f32),
            pltpu.VMEM((edges,) + plane, f32), *[pltpu.VMEM((blocks,) + plane, f32)] * edges,
            pltpu.VMEM((4,) + plane, f32), pltpu.VMEM((2,) + plane, f32),
            pltpu.VMEM((2 * SWEEPS_FINE, subs) + plane, f32),
            pltpu.VMEM((subs, blocks, payload, LANES), f32),
            pltpu.VMEM((NV * planes, LANES), f32),
            pltpu.SMEM((blocks,), jnp.int32),
            mid, mid, mid, mid, mid, low, low, low, low, low,
            pltpu.VMEM((NV * planes, LANES), f32),
            dma((edges, blocks)), dma((edges, blocks)), dma((3,)), dma((3,)),
            dma((2 * SWEEPS_FINE, subs)), dma((2 * SWEEPS_FINE, subs)),
            dma((blocks,)), dma((blocks,)), dma((subs, blocks)), dma((subs, blocks)),
        ],
        compiler_params=pltpu.CompilerParams(collective_id=0, has_side_effects=True, vmem_limit_bytes=60 * 1024 * 1024),
    )(tiled(solution), tiled(right_side), couple.transpose(2, 3, 0, 1), partner, orient, owner_one, owner_two)
    corrected, one, two, norms = pl.pallas_call(
        finish,
        name="finish",
        out_shape=(
            jax.ShapeDtypeStruct((NV, 1, planes, cells), f32),
            jax.ShapeDtypeStruct((NV, 1, planes // 2, cells // 4), f32),
            jax.ShapeDtypeStruct((NV, 1, planes // 4, cells // 16), f32),
            jax.ShapeDtypeStruct((3,), f32),
        ),
        in_specs=[vmem] * 4,
        out_specs=(vmem, vmem, vmem, smem),
    )(*[pltpu.with_memory_space_constraint(x, pltpu.VMEM) for x in (corrected, one, two, norms)])
    return corrected, one, two, norms


def solution(mesh):
    split = P(None, "blk", "sub", None)
    return jax.shard_map(
        shards,
        mesh=mesh,
        in_specs=(split, split, P(), P(), P(), P(), P()),
        out_specs=(split, split, split, P()),
        check_vma=False,
    )
```

```python
import functools

import jax
import jax.numpy as jnp
from jax import lax
from jax.experimental import pallas as pl
from jax.experimental.pallas import tpu as pltpu
from jax.sharding import PartitionSpec as P

BI = 32
BJ = 16
SWEEPS_FINE = 2
SWEEPS_MID = 2
SWEEPS_COARSE = 4
LANES = 128
SUBLANES = 8
NV = 5
MESH = pl.DeviceIdType.MESH

RAW = 0
INV, IM, IP, JM, JP, FWD, BWD = 7, 8, 9, 10, 11, 12, 13
F2, F4, F8, FP, B2, B4, B8, BP = 14, 15, 16, 17, 18, 19, 20, 21
F16, B16, G0, G1 = 22, 23, 24, 25


def product(left, right):
    total = left[0][None] * right[:, 0][:, None]
    for b in range(1, NV):
        total = total + left[b][None] * right[:, b][:, None]
    return total


def permute(values, places):
    flat = values.reshape(-1, LANES)
    index = jnp.broadcast_to(places, values.shape).reshape(-1, LANES)
    return jnp.take_along_axis(flat, index, axis=1, mode="promise_in_bounds").reshape(values.shape)


def halves(values):
    high = values.astype(jnp.bfloat16)
    return high, (values - high.astype(jnp.float32)).astype(jnp.bfloat16)


def chosen(values, selection):
    high, low = halves(values)
    picks = selection.astype(jnp.bfloat16)
    return (jnp.dot(high, picks, preferred_element_type=jnp.float32)
            + jnp.dot(low, picks, preferred_element_type=jnp.float32))


def kernel(
    sizes, solution, right_side, couple, partner, orient, owner_one, owner_two,
    corrected, out_one, out_two, norms,
    coef, coef_one, coef_two, cg, sf, yf, tf, zf, wide, old_above,
    xsend, *more,
):
    edges = SWEEPS_FINE + 1
    edge_w, edge_a, more = more[:edges], more[edges:2 * edges], more[2 * edges:]
    (
        starts, prefix, gathered, rsum, low_recv, squares_recv,
        down,
        field_f, field_c, field_p, field_v, field_y,
        two_f, two_c, two_p, two_v, two_y, spread,
        xs_sem, xw_sem, xa_sem, us_sem, ur_sem, ps_sem, pr_sem, gs_sem, gr_sem, es_sem, er_sem,
        hs_sem, hr_sem, ns_sem, nr_sem,
    ) = more
    blocks, subs = sizes
    me = lax.axis_index("blk")
    sub = lax.axis_index("sub")
    last = subs - 1
    is_low = sub == 0
    is_high = sub == last
    rows = solution.shape[1]
    planes = SUBLANES
    count_all = blocks * subs
    here = me * subs + sub

    @pl.loop(1, count_all)
    def _(step):
        there = (here + step) % count_all
        pl.semaphore_signal(pltpu.get_barrier_semaphore(), inc=1,
                            device_id=(there // subs, there % subs), device_id_type=MESH)

    def found(mapping, value):
        return lax.fori_loop(0, blocks, lambda n, best: jnp.where(mapping[n] == value, n, best), 0)

    @pl.loop(0, blocks)
    def _(n):
        down[n] = found(partner, n)

    held = (found(owner_one, me), found(owner_two, me))
    lane = lax.broadcasted_iota(jnp.int32, (1, LANES), 1)
    place = lax.broadcasted_iota(jnp.int32, (SUBLANES, LANES), 0)

    def edge_copy(n, b, t, kind, source):
        edge = edge_a if kind else edge_w
        return pltpu.make_async_remote_copy(
            src_ref=xsend.at[n], dst_ref=edge[n].at[source], send_sem=xs_sem.at[n, b, t],
            recv_sem=(xa_sem if kind else xw_sem).at[n, source], device_id=(b, t), device_id_type=MESH)

    def targets(n, kind):
        if n < SWEEPS_FINE:
            return (0, last) + tuple(range(1, last))
        return (last,) if kind else (0,)

    def send_edge(n, ref):
        code = jnp.where(is_low, orient[down[me]], orient[me])
        turned = permute(ref[...], lane ^ jnp.where(code // 2 == 1, BJ - 1, 0) ^ jnp.where(code % 2 == 1, LANES - BJ, 0))
        swapped = jnp.concatenate([turned[:, r:r + 1] for r in range(rows - 1, -1, -1)], axis=1)
        turned = jnp.where(code % 2 == 1, swapped, turned)

        for kind, mine in ((1, is_low), (0, is_high)):
            @pl.when(mine)
            def _():
                edge = edge_a if kind else edge_w
                at = 0 if kind else planes - 1
                xsend[n] = turned[:, :, at:at + 1]
                edge[n][me] = turned[:, :, at:at + 1]
                own = 0 if kind else last
                for t in targets(n, kind):
                    first = 1 if t == own else 0

                    @pl.loop(first, blocks)
                    def _(step):
                        edge_copy(n, (me + step) % blocks, t, kind, me).start()

    def receive_edge(n):
        for kind in (0, 1):
            own = 0 if kind else last
            for t in range(subs):
                if t not in targets(n, kind):
                    continue
                first = 1 if t == own else 0

                @pl.when(sub == t)
                def _():
                    @pl.loop(first, blocks)
                    def _(step):
                        source = (me + step) % blocks
                        edge_copy(n, source, t, kind, source).wait_recv()

    def start_copy(source, target):
        return pltpu.make_async_remote_copy(
            src_ref=starts.at[source], dst_ref=starts.at[source], send_sem=us_sem.at[target],
            recv_sem=ur_sem.at[source], device_id=(me, target), device_id_type=MESH)

    def prefix_copy(n, source, target):
        return pltpu.make_async_remote_copy(
            src_ref=prefix.at[n, source], dst_ref=prefix.at[n, source], send_sem=ps_sem.at[n, target],
            recv_sem=pr_sem.at[n, source], device_id=(me, target), device_id_type=MESH)

    def splat(level, matrix):
        return jnp.stack([
            jnp.stack([jnp.full((SUBLANES, LANES), couple[a, b, level, matrix], jnp.float32) for a in range(NV)])
            for b in range(NV)
        ])

    identity = jnp.stack([
        jnp.stack([jnp.full((SUBLANES, LANES), 1.0 if a == b else 0.0, jnp.float32) for a in range(NV)])
        for b in range(NV)
    ])

    def prepare(level, store):
        for matrix in range(7):
            store[RAW + matrix] = splat(level, matrix)
        store[INV] = identity

        @pl.loop(0, 6)
        def _(repeat):
            approx = store[INV]
            store[INV] = product(approx, 2.0 * identity - product(store[RAW], approx))

        @pl.loop(0, 6)
        def _(matrix):
            store[IM + matrix] = product(store[INV], store[RAW + 1 + matrix])

    prepare(0, coef)

    def powers(base, second, sixteenth, count):
        coef[second] = product(coef[base], coef[base])
        coef[second + 1] = product(coef[second], coef[second])
        coef[second + 2] = product(coef[second + 1], coef[second + 1])
        coef[sixteenth] = product(coef[second + 2], coef[second + 2])
        run = jnp.where((count & 1) != 0, coef[base], identity)
        for bit, index in ((2, second), (4, second + 1), (8, second + 2)):
            run = product(jnp.where((count & bit) != 0, coef[index], identity), run)
        coef[second + 3] = run

    powers(FWD, F2, F16, place + 1)
    powers(BWD, B2, B16, planes - place)

    def combined():
        seventh = product(coef[B4], product(coef[B2], coef[BWD]))

        @pl.loop(0, NV)
        def _(n):
            middle = jnp.where(n == 0, identity, coef[jnp.maximum(IM + n - 1, IM)])
            total = product(middle, coef[FWD])
            for back, ahead in ((BWD, FWD), (B2, F2), (B4, F4)):
                total = total + product(coef[back], product(total, coef[ahead]))
            coef[G0 + n] = jnp.where(place < subs, total, product(seventh, middle))

    def apply(index, values, height=SUBLANES):
        total = None
        for b in range(NV):
            term = coef[index, b][:, None, :height] * values[b][None]
            total = term if total is None else total + term
        return total

    in_low = lane < BJ
    in_high = lane >= LANES - BJ
    j_first = (lane & (BJ - 1)) == 0
    j_final = (lane & (BJ - 1)) == BJ - 1

    def lateral(values, base):
        zero = jnp.zeros_like(values[:, :1])
        turned = pltpu.roll(values, BJ, 3)
        total = apply(base, jnp.where(in_low, jnp.concatenate([zero, turned[:, :-1]], axis=1), turned))
        turned = pltpu.roll(values, LANES - BJ, 3)
        total = total + apply(base + 1, jnp.where(in_high, jnp.concatenate([turned[:, 1:], zero], axis=1), turned))
        total = total + apply(base + 2, jnp.where(j_first, 0.0, pltpu.roll(values, 1, 3)))
        return total + apply(base + 3, jnp.where(j_final, 0.0, pltpu.roll(values, LANES - 1, 3)))

    def scan(values, indices, reverse, length=planes):
        by = 1
        for index in indices:
            if reverse:
                shifted = jnp.where(place < length - by, pltpu.roll(values, SUBLANES - by, 2), 0.0)
            else:
                shifted = jnp.where((place >= by) & (place < length), pltpu.roll(values, by, 2), 0.0)
            values = values + apply(index, shifted)
            by *= 2
        return values

    starts[sub] = solution[:, :, 0:1, :]
    cg[...] = apply(INV, right_side[...])
    upper = jnp.where(place == planes - 1, 0.0, pltpu.roll(solution[...], planes - 1, 2))
    sf[...] = cg[...] + lateral(solution[...], IM) + apply(BWD, upper)

    def local(n):
        yf[...] = scan(sf[...], (FWD, F2, F4), False)
        tf[...] = cg[...] + lateral(yf[...], IM) + (yf[...] - sf[...])
        part = scan(tf[...], (BWD, B2, B4), True)
        prefix[n, sub, 0] = yf[:, :, planes - 1:planes, :]
        prefix[n, sub, 1] = part[:, :, 0:1, :]

    def send_prefix(n):
        for target in range(subs):
            @pl.when(sub != target)
            def _():
                prefix_copy(n, sub, target).start()

    local(0)
    pl.semaphore_wait(pltpu.get_barrier_semaphore(), count_all - 1)
    send_edge(0, solution)
    for target in range(subs):
        @pl.when((sub > 0) & (sub != target))
        def _():
            start_copy(sub, target).start()
    send_prefix(0)
    combined()
    for number, store in ((1, coef_one), (2, coef_two)):
        prepare(number, store)
        width = BJ >> number
        cells = rows * LANES >> (2 * number)
        inside = lane < cells
        masks = ((lane >= width) & inside, lane < cells - width,
                 ((lane & (width - 1)) != 0) & inside, ((lane & (width - 1)) != width - 1) & inside)
        for shift, mask in enumerate(masks):
            for base in (RAW + 1, IM):
                store[base + shift] = jnp.where(mask, store[base + shift], 0.0)

    for n in range(SWEEPS_FINE):
        for source in range(subs):
            @pl.when(sub != source)
            def _():
                if n == 0 and source > 0:
                    start_copy(source, sub).wait_recv()
                prefix_copy(n, source, sub).wait_recv()
        receive_edge(n)
        below = edge_w[n][down[me]]
        above = edge_a[n][partner[me]]
        missing = above if n == 0 else above - old_above[...]
        ahead = jnp.where(place == subs + last, missing, 0.0)
        if n == 0:
            for s in range(last):
                ahead = jnp.where(place == subs + s, starts[s + 1], ahead)
        old_above[...] = above
        ahead = apply(BWD, ahead)
        enter = jnp.where(place == 0, below, 0.0)
        final = jnp.zeros_like(enter)
        for s in range(subs):
            if s < last:
                enter = jnp.where(place == s + 1, prefix[n, s, 0], enter)
            if s > 0:
                final = jnp.where(place == s, prefix[n, s, 1], final)
        moved = pltpu.roll(ahead, SUBLANES + 1 - subs, 2)
        enter = enter + jnp.where((place > 0) & (place < subs), moved, 0.0)
        enter = scan(enter, (F8, F16), False, subs)
        both = enter + ahead
        sides = lateral(both, G1)
        final = final + apply(G0, enter) + sides + pltpu.roll(sides, SUBLANES - subs, 2)
        final = jnp.where(place < last, pltpu.roll(final, SUBLANES - 1, 2), jnp.where(place == last, above, 0.0))
        final = scan(final, (B8, B16), True, subs)
        wide[0] = both
        wide[1] = final
        enter = wide[0, :, :, pl.ds(sub, 1), :]
        extra = jnp.where(place == planes - 1, wide[0, :, :, pl.ds(subs + sub, 1), :], 0.0)
        y = yf[...] + apply(FP, enter) + extra
        yf[...] = y
        tf[...] = cg[...] + lateral(y, IM) + (y - (sf[...] + extra))
        zf[...] = scan(tf[...], (BWD, B2, B4), True) + apply(BP, wide[1, :, :, pl.ds(sub, 1), :])
        if n + 1 < SWEEPS_FINE:
            send_edge(n + 1, zf)
            sf[...] = cg[...] + lateral(zf[...], IM) + (zf[...] - tf[...])
            local(n + 1)
            send_prefix(n + 1)

    change = zf[...] - yf[...]
    lower = jnp.where(place == 0, -wide[0, :, :, pl.ds(sub, 1), :], pltpu.roll(change, 1, 2))
    upper = jnp.where((place == planes - 1) & is_high, -old_above[...], 0.0)
    sf[...] = lateral(change, RAW + 1) + apply(RAW + 5, lower) + apply(RAW + 6, upper)

    height = rows * LANES
    r_row = lax.broadcasted_iota(jnp.int32, (height, LANES), 0)
    r_col = lax.broadcasted_iota(jnp.int32, (height, LANES), 1)
    half = BJ // 2
    share = ((((r_row >> 5) * half) + ((r_row & (BJ - 1)) >> 1)) == r_col).astype(jnp.float32)
    reduced = None
    for r in range(rows):
        both = jnp.concatenate([sf[:, r].reshape(NV * SUBLANES, LANES), zf[:, r].reshape(NV * SUBLANES, LANES)], axis=0)
        term = chosen(both, share[r * LANES:(r + 1) * LANES])
        reduced = term if reduced is None else reduced + term
    count = NV * planes // 2
    rsum[...] = reduced * 0.125
    gathered[sub, me, 0:count, :] = rsum[pl.ds(0, count, stride=2), :] + rsum[pl.ds(1, count, stride=2), :]
    tail = gathered.shape[2] - count - 2 * NV
    gathered[sub, me, count:count + NV, :] = rsum[pl.ds(NV * planes + planes - 1, NV, stride=planes), :]
    gathered[sub, me, count + NV:count + 2 * NV, :] = rsum[pl.ds(NV * planes, NV, stride=planes), :]
    gathered[sub, me, count + 2 * NV:, :] = jnp.zeros((tail, LANES), jnp.float32)

    def spread_copy(source, target):
        return pltpu.make_async_remote_copy(
            src_ref=gathered.at[sub, source], dst_ref=gathered.at[sub, source], send_sem=gs_sem.at[target],
            recv_sem=gr_sem.at[source], device_id=(target, sub), device_id_type=MESH)

    @pl.loop(1, blocks)
    def _(step):
        spread_copy(me, (me + step) % blocks).start()

    def across_copy(source, block, target):
        return pltpu.make_async_remote_copy(
            src_ref=gathered.at[source, block], dst_ref=gathered.at[source, block],
            send_sem=es_sem.at[target, block], recv_sem=er_sem.at[source, block],
            device_id=(me, target), device_id_type=MESH)

    for step in range(1, subs):
        across_copy(sub, me, (sub + step) % subs).start()

    @pl.loop(1, blocks)
    def _(step):
        source = (me + step) % blocks
        spread_copy(source, source).wait_recv()
        for turn in range(1, subs):
            across_copy(sub, source, (sub + turn) % subs).start()

    @pl.loop(0, blocks)
    def _(block):
        for turn in range(1, subs):
            source = (sub + turn) % subs
            across_copy(source, block, source).wait_recv()

    send_edge(SWEEPS_FINE, zf)
    low_recv[0] = zf[:, :, planes - 1:planes, :]

    def halo_copy(target):
        return pltpu.make_async_remote_copy(
            src_ref=low_recv.at[0], dst_ref=low_recv.at[1], send_sem=hs_sem.at[0], recv_sem=hr_sem.at[0],
            device_id=(me, target), device_id_type=MESH)

    @pl.when(jnp.logical_not(is_high))
    def _():
        halo_copy(sub + 1).start()

    def use(store, index, values):
        cut = values.reshape(NV, -1, SUBLANES, LANES)
        terms = [store[index, b][:, None] * cut[b][None] for b in range(NV)]
        out = (terms[0] + terms[1]) + (terms[2] + terms[3]) + terms[4]
        return out.reshape(values.shape)

    slot = lax.broadcasted_iota(jnp.int32, (blocks, 1), 0)

    def codes(source):
        out = jnp.zeros((blocks, 1), jnp.int32)
        for n in range(blocks):
            out = jnp.where(slot == n, source(n), out)
        return out

    code_below = codes(lambda n: orient[down[n]])
    code_above = codes(lambda n: orient[n])

    def turned(values, code, cells, width):
        high = jnp.where((code & 1) != 0, cells - width, 0)
        return permute(values, lane ^ high ^ jnp.where(code >= 2, width - 1, 0))

    local_planes = planes // 2
    cells_one = rows * LANES // 4

    def edge_rows(s, pick, first):
        return jnp.stack([
            jnp.concatenate([gathered[s, pl.ds(pick(n), 1), first + a, :] for n in range(blocks)], axis=0)
            for a in range(NV)])

    under = turned(edge_rows(last, lambda n: down[n], count), code_below, cells_one, BJ // 2)
    over = turned(edge_rows(0, lambda n: partner[n], count + NV), code_above, cells_one, BJ // 2)
    for s in range(subs):
        if s > 0:
            under = jnp.stack([gathered[s - 1, :, count + a, :] for a in range(NV)])
        under = use(coef, RAW + 5, under)
        for k in range(local_planes):
            value = jnp.stack([gathered[s, :, a * local_planes + k, :] for a in range(NV)])
            if k == 0:
                value = value + under
            if s == last and k == local_planes - 1:
                value = value + use(coef, RAW + 6, over)
            field_f[:, s * local_planes + k] = value

    def root_mean(value, entries):
        return jnp.sqrt(jnp.sum(value, axis=1, keepdims=True) / jnp.float32(entries))

    size = NV * blocks * subs * planes * rows * LANES

    def level(store, cells, width, g, c, p, v, y, sweeps):
        depth = g.shape[1]
        chunk = max(1, 4 * SUBLANES // blocks)
        steps = depth // chunk

        def repeat(body, start, number):
            return lax.fori_loop(0, number, body, start, unroll=blocks <= SUBLANES)

        def sides(values, base):
            axis = values.ndim - 1
            out = use(store, base, pltpu.roll(values, width, axis))
            out = out + use(store, base + 1, pltpu.roll(values, LANES - width, axis))
            out = out + use(store, base + 2, pltpu.roll(values, 1, axis))
            return out + use(store, base + 3, pltpu.roll(values, LANES - 1, axis))

        def interfaces():
            below = jnp.concatenate([v[:, depth - 1, pl.ds(down[n], 1), :] for n in range(blocks)], axis=1)
            above = jnp.concatenate([v[:, 0, pl.ds(partner[n], 1), :] for n in range(blocks)], axis=1)
            return turned(below, code_below, cells, width), turned(above, code_above, cells, width)

        def centre(step, carry):
            at = pl.ds(step * chunk, chunk)
            c[:, at] = use(store, INV, g[:, at])
            return carry

        repeat(centre, 0, steps)
        nothing = jnp.zeros((NV, blocks, LANES), jnp.float32)
        below, above = nothing, nothing
        for n in range(sweeps):
            if n > 0:
                below, above = interfaces()
                p[:, depth - 1] = use(store, BWD, above)

            def forward(step, previous):
                at = pl.ds(step * chunk, chunk)
                s = c[:, at]
                if n > 0:
                    s = s + sides(v[:, at], IM) + p[:, at]
                made = []
                for u in range(chunk):
                    behind = use(store, FWD, previous)
                    previous = s[:, u] + behind
                    made.append((previous, behind))
                for u, (now, behind) in enumerate(made):
                    y[:, step * chunk + u] = now
                    p[:, step * chunk + u] = behind
                return previous

            repeat(forward, below, steps)

            def backward(step, following):
                start = depth - chunk - step * chunk
                at = pl.ds(start, chunk)
                t = c[:, at] + sides(y[:, at], IM) + p[:, at]
                made = []
                for u in range(chunk - 1, -1, -1):
                    ahead = use(store, BWD, following)
                    following = t[:, u] + ahead
                    made.append((u, following, ahead))
                for u, now, ahead in made:
                    v[:, start + u] = now
                    p[:, start + u] = ahead
                return following

            repeat(backward, above, steps)

        new_below, new_above = interfaces()
        top = use(store, RAW + 6, new_above - above)

        def remain(step, carry, final=False):
            squares, previous = carry
            at = pl.ds(step * chunk, chunk)
            change = v[:, at] - y[:, at]
            shifted = jnp.stack([previous] + [change[:, u] for u in range(chunk - 1)], axis=1)
            out = sides(change, RAW + 1) + use(store, RAW + 5, shifted)
            if final:
                out = jnp.stack([out[:, u] for u in range(chunk - 1)] + [out[:, chunk - 1] + top], axis=1)
            c[:, at] = out
            return squares + jnp.sum(out * out, axis=1), change[:, chunk - 1]

        carry = repeat(remain, (nothing, new_below - below), steps - 1)
        squares, _ = remain(steps - 1, carry, True)
        return jnp.sum(squares.reshape(NV * blocks, LANES), axis=0, keepdims=True)

    depth_one = field_f.shape[1]
    total = level(coef_one, cells_one, BJ // 2, field_f, field_c, field_p, field_v, field_y, SWEEPS_MID)
    norms[1:2, :] = jnp.broadcast_to(root_mean(total, size // 8), (1, LANES))

    receive_edge(SWEEPS_FINE)

    @pl.when(is_low)
    def _():
        low_recv[1] = edge_w[SWEEPS_FINE][down[me]]

    @pl.when(is_high)
    def _():
        fresh = apply(RAW + 6, edge_a[SWEEPS_FINE][partner[me]], 1)
        sf[:, :, planes - 1:planes, :] = sf[:, :, planes - 1:planes, :] + fresh

    @pl.when(jnp.logical_not(is_low))
    def _():
        halo_copy(sub).wait_recv()

    sf[:, :, 0:1, :] = sf[:, :, 0:1, :] + apply(RAW + 5, low_recv[1], 1)
    residual = sf[...]
    squares_recv[here] = jnp.sum((residual * residual).reshape(NV * rows * SUBLANES, LANES), axis=0, keepdims=True)

    def norm_copy(source, target):
        return pltpu.make_async_remote_copy(
            src_ref=squares_recv.at[source], dst_ref=squares_recv.at[source], send_sem=ns_sem.at[target],
            recv_sem=nr_sem.at[source], device_id=(target // subs, target % subs), device_id_type=MESH)

    @pl.loop(1, count_all)
    def _(step):
        norm_copy(here, (here + step) % count_all).start()

    s_row = lax.broadcasted_iota(jnp.int32, (LANES, LANES), 0)
    s_col = lax.broadcasted_iota(jnp.int32, (LANES, LANES), 1)
    fold = ((((s_row >> 4) * (BJ // 4)) + ((s_row & (BJ // 2 - 1)) >> 1)) == s_col).astype(jnp.float32)
    depth_two = depth_one // 2

    pairs = jnp.stack([field_c[:, 2 * k] + field_c[:, 2 * k + 1] for k in range(depth_two)], axis=1)
    two_f[...] = chosen(pairs.reshape(-1, LANES) * 0.125, fold).reshape(two_f.shape)

    total = level(coef_two, cells_one // 4, BJ // 4, two_f, two_c, two_p, two_v, two_y, SWEEPS_COARSE)
    norms[2:3, :] = jnp.broadcast_to(root_mean(total, size // 64), (1, LANES))

    unfold = ((((s_col >> 4) * (BJ // 4)) + ((s_col & (BJ // 2 - 1)) >> 1)) == s_row).astype(jnp.float32)
    coarse_planes = local_planes // 2
    for which, block in enumerate((me, held[0])):
        for a in range(NV):
            for k in range(coarse_planes):
                row = (which * NV + a) * coarse_planes + k
                rsum[row:row + 1, :] = two_v[a, sub * coarse_planes + k, pl.ds(block, 1), :]
    for a in range(NV):
        for k in range(coarse_planes):
            out_two[a, pl.ds(k, 1), :] = two_v[a, sub * coarse_planes + k, pl.ds(held[1], 1), :]
    filled = -(-2 * NV * coarse_planes // SUBLANES) * SUBLANES
    rsum[0:filled, :] = chosen(rsum[0:filled, :], unfold)
    for a in range(NV):
        for k in range(local_planes):
            at = sub * local_planes + k
            mine = a * coarse_planes + k // 2
            row = field_v[a, at, pl.ds(me, 1), :] + rsum[mine:mine + 1, :]
            spread[pl.ds(a * planes + 2 * k, 2), :] = jnp.broadcast_to(row, (2, LANES))
            mine = mine + NV * coarse_planes
            out_one[a, pl.ds(k, 1), :] = field_v[a, at, pl.ds(held[0], 1), :] + rsum[mine:mine + 1, :]

    for r in range(rows):
        grow = ((((s_col + r * LANES) >> 5) * half) + ((s_col & (BJ - 1)) >> 1) == s_row).astype(jnp.float32)
        corrected[:, r] = zf[:, r] + chosen(spread[...], grow).reshape(NV, SUBLANES, LANES)

    @pl.loop(1, count_all)
    def _(step):
        source = (here + step) % count_all
        norm_copy(source, source).wait_recv()

    total = jnp.sum(squares_recv[...].reshape(count_all, LANES), axis=0, keepdims=True)
    norms[0:1, :] = jnp.broadcast_to(root_mean(total, size), (1, LANES))

    for n in range(SWEEPS_FINE + 1):
        for kind, mine in ((1, is_low), (0, is_high)):
            @pl.when(mine)
            def _():
                own = 0 if kind else last
                for t in targets(n, kind):
                    first = 1 if t == own else 0

                    @pl.loop(first, blocks)
                    def _(step):
                        edge_copy(n, (me + step) % blocks, t, kind, me).wait_send()

    for target in range(subs):
        @pl.when((sub > 0) & (sub != target))
        def _():
            start_copy(sub, target).wait_send()

        @pl.when(sub != target)
        def _():
            for n in range(SWEEPS_FINE):
                prefix_copy(n, sub, target).wait_send()

    @pl.when(jnp.logical_not(is_high))
    def _():
        halo_copy(sub + 1).wait_send()

    @pl.loop(1, blocks)
    def _(step):
        spread_copy(me, (me + step) % blocks).wait_send()

    @pl.loop(0, blocks)
    def _(block):
        for turn in range(1, subs):
            across_copy(sub, block, (sub + turn) % subs).wait_send()

    @pl.loop(1, count_all)
    def _(step):
        norm_copy(here, (here + step) % count_all).wait_send()


def finish(corrected, one, two, norms, out, out_one, out_two, out_norms):
    for r in range(corrected.shape[1]):
        out[:, 0, :, r * LANES:(r + 1) * LANES] = corrected[:, r]
    out_one[:, 0] = one[...]
    out_two[:, 0] = two[:, :, :out_two.shape[3]]
    for n in range(3):
        out_norms[n] = jnp.max(norms[n:n + 1, :])


def shards(solution, right_side, couple, partner, orient, owner_one, owner_two):
    blocks = lax.axis_size("blk")
    subs = lax.axis_size("sub")
    planes, cells = solution.shape[2:]
    rows = cells // LANES
    tall = planes * subs

    def tiled(x):
        return x.reshape(NV, planes, rows, LANES).transpose(0, 2, 1, 3)

    vmem = pl.BlockSpec(memory_space=pltpu.VMEM)
    smem = pl.BlockSpec(memory_space=pltpu.SMEM)
    f32 = jnp.float32
    fine = pltpu.VMEM((NV, rows, planes, LANES), f32)
    plane = (NV, rows, 1, LANES)
    mid = pltpu.VMEM((NV, tall // 2, blocks, LANES), f32)
    low = pltpu.VMEM((NV, tall // 4, blocks, LANES), f32)
    matrix = (NV, NV, SUBLANES, LANES)
    payload = -(-(NV * planes // 2 + 2 * NV) // SUBLANES) * SUBLANES
    dma = pltpu.SemaphoreType.DMA
    edges = SWEEPS_FINE + 1
    everyone = blocks * subs
    results = pl.pallas_call(
        functools.partial(kernel, (blocks, subs)),
        name="vcycle",
        out_shape=(
            pltpu.VMEM((NV, rows, planes, LANES), f32),
            pltpu.VMEM((NV, planes // 2, LANES), f32),
            pltpu.VMEM((NV, planes // 4, LANES), f32),
            pltpu.VMEM((3, LANES), f32),
        ),
        in_specs=[vmem, vmem, smem, smem, smem, smem, smem],
        out_specs=(vmem, vmem, vmem, vmem),
        scratch_shapes=[
            pltpu.VMEM((29,) + matrix, f32), pltpu.VMEM((14,) + matrix, f32), pltpu.VMEM((14,) + matrix, f32),
            fine, fine, fine, fine, fine, pltpu.VMEM((2, NV, rows, planes, LANES), f32), pltpu.VMEM(plane, f32),
            pltpu.VMEM((edges,) + plane, f32),
            *[pltpu.VMEM((blocks,) + plane, f32)] * (2 * edges),
            pltpu.VMEM((subs,) + plane, f32),
            pltpu.VMEM((SWEEPS_FINE, subs, 2) + plane, f32),
            pltpu.VMEM((subs, blocks, payload, LANES), f32),
            pltpu.VMEM((2 * NV * planes, LANES), f32),
            pltpu.VMEM((2,) + plane, f32),
            pltpu.VMEM((everyone, 1, LANES), f32),
            pltpu.SMEM((blocks,), jnp.int32),
            mid, mid, mid, mid, mid, low, low, low, low, low,
            pltpu.VMEM((NV * planes, LANES), f32),
            dma((edges, blocks, subs)), dma((edges, blocks)), dma((edges, blocks)),
            dma((subs,)), dma((subs,)),
            dma((SWEEPS_FINE, subs)), dma((SWEEPS_FINE, subs)),
            dma((blocks,)), dma((blocks,)), dma((subs, blocks)), dma((subs, blocks)),
            dma((1,)), dma((1,)), dma((everyone,)), dma((everyone,)),
        ],
        compiler_params=pltpu.CompilerParams(collective_id=0, has_side_effects=True, vmem_limit_bytes=60 * 1024 * 1024),
    )(tiled(solution), tiled(right_side), couple.transpose(2, 3, 0, 1), partner, orient, owner_one, owner_two)
    return pl.pallas_call(
        finish,
        name="finish",
        out_shape=(
            jax.ShapeDtypeStruct((NV, 1, planes, cells), f32),
            jax.ShapeDtypeStruct((NV, 1, planes // 2, cells // 4), f32),
            jax.ShapeDtypeStruct((NV, 1, planes // 4, cells // 16), f32),
            jax.ShapeDtypeStruct((3,), f32),
        ),
        in_specs=[vmem] * 4,
        out_specs=(vmem, vmem, vmem, smem),
    )(*[pltpu.with_memory_space_constraint(x, pltpu.VMEM) for x in results])


def solution(mesh):
    split = P(None, "blk", "sub", None)
    return jax.shard_map(
        shards,
        mesh=mesh,
        in_specs=(split, split, P(), P(), P(), P(), P()),
        out_specs=(split, split, split, P()),
        check_vma=False,
    )
```

```python
import functools

import jax
import jax.numpy as jnp
from jax import lax
from jax.experimental import pallas as pl
from jax.experimental.pallas import tpu as pltpu
from jax.sharding import PartitionSpec as P

BI = 32
BJ = 16
SWEEPS_FINE = 2
SWEEPS_MID = 2
SWEEPS_COARSE = 4
LANES = 128
SUBLANES = 8
NV = 5
MESH = pl.DeviceIdType.MESH

RAW = 0
INV, IM, IP, JM, JP, FWD, BWD = 7, 8, 9, 10, 11, 12, 13
F2, F4, F8, FP, B2, B4, B8, BP = 14, 15, 16, 17, 18, 19, 20, 21
F16, B16, G0, G1 = 22, 23, 24, 25


def product(left, right):
    total = left[0][None] * right[:, 0][:, None]
    for b in range(1, NV):
        total = total + left[b][None] * right[:, b][:, None]
    return total


def permute(values, places):
    flat = values.reshape(-1, LANES)
    index = jnp.broadcast_to(places, values.shape).reshape(-1, LANES)
    return jnp.take_along_axis(flat, index, axis=1, mode="promise_in_bounds").reshape(values.shape)


def halves(values):
    high = values.astype(jnp.bfloat16)
    return high, (values - high.astype(jnp.float32)).astype(jnp.bfloat16)


def chosen(values, selection):
    high, low = halves(values)
    picks = selection.astype(jnp.bfloat16)
    return (jnp.dot(high, picks, preferred_element_type=jnp.float32)
            + jnp.dot(low, picks, preferred_element_type=jnp.float32))


def kernel(
    sizes, solution_hbm, right_side_hbm, couple_hbm, partner_hbm, orient_hbm, owner_one_hbm, owner_two_hbm,
    corrected, out_one, out_two, norms,
    coef, coef_one, coef_two, cg, sf, yf, tf, zf, wide, old_above,
    xsend, *more,
):
    edges = SWEEPS_FINE + 1
    edge_w, edge_a, more = more[:edges], more[edges:2 * edges], more[2 * edges:]
    (
        starts, prefix, gathered, rsum, low_recv, squares_recv,
        down,
        field_f, field_c, field_p, field_v, field_y,
        two_f, two_c, two_p, two_v, two_y, spread,
        xs_sem, xw_sem, xa_sem, us_sem, ur_sem, ps_sem, pr_sem, gs_sem, gr_sem, es_sem, er_sem,
        hs_sem, hr_sem, ns_sem, nr_sem, solution, right_side, couple, partner, orient, owner_one, owner_two, in_sem,
    ) = more
    blocks, subs = sizes
    me = lax.axis_index("blk")
    sub = lax.axis_index("sub")
    last = subs - 1
    is_low = sub == 0
    is_high = sub == last
    rows = solution.shape[1]
    planes = SUBLANES
    count_all = blocks * subs
    here = me * subs + sub
    fetch = [pltpu.make_async_copy(source, target, in_sem.at[n]) for n, (source, target) in enumerate(
        ((solution_hbm, solution), (right_side_hbm, right_side), (couple_hbm, couple), (partner_hbm, partner),
         (orient_hbm, orient), (owner_one_hbm, owner_one), (owner_two_hbm, owner_two)))]
    for copy in fetch:
        copy.start()

    def after(index, step, length):
        return jnp.where(index + step >= length, index + step - length, index + step)

    def everyone(body):
        for turn in range(subs):
            part = after(sub, turn, subs)

            @pl.loop(0 if turn else 1, blocks)
            def _(step):
                body(after(me, step, blocks), part)

    everyone(lambda b, t: pl.semaphore_signal(
        pltpu.get_barrier_semaphore(), inc=1, device_id=(b, t), device_id_type=MESH))
    for copy in fetch[3:]:
        copy.wait()

    def found(mapping, value):
        return lax.fori_loop(0, blocks, lambda n, best: jnp.where(mapping[n] == value, n, best), 0)

    @pl.loop(0, blocks)
    def _(n):
        down[n] = found(partner, n)

    held = (found(owner_one, me), found(owner_two, me))
    lane = lax.broadcasted_iota(jnp.int32, (1, LANES), 1)
    place = lax.broadcasted_iota(jnp.int32, (SUBLANES, LANES), 0)

    def edge_copy(n, b, t, kind, source):
        edge = edge_a if kind else edge_w
        return pltpu.make_async_remote_copy(
            src_ref=xsend.at[n], dst_ref=edge[n].at[source], send_sem=xs_sem.at[n, b, t],
            recv_sem=(xa_sem if kind else xw_sem).at[n, source], device_id=(b, t), device_id_type=MESH)

    def targets(n, kind):
        if n < SWEEPS_FINE:
            return (0, last) + tuple(range(1, last))
        return (last,) if kind else (0,)

    ends = ((1, is_low, 0, 0), (0, is_high, last, planes - 1))

    def stage_edge(n, ref):
        for kind, mine, own, at in ends:
            @pl.when(mine)
            def _():
                code = orient[down[me]] if kind else orient[me]
                places = lane ^ jnp.where(code // 2 == 1, BJ - 1, 0) ^ jnp.where(code % 2 == 1, LANES - BJ, 0)
                moved = permute(ref[...], places)
                swapped = jnp.concatenate([moved[:, r:r + 1] for r in range(rows - 1, -1, -1)], axis=1)
                moved = jnp.where(code % 2 == 1, swapped, moved)[:, :, at:at + 1]
                xsend[n] = moved
                (edge_a if kind else edge_w)[n][me] = moved

    def each_edge(n, act):
        for kind, mine, own, at in ends:
            @pl.when(mine)
            def _():
                for t in targets(n, kind):
                    @pl.loop(1 if t == own else 0, blocks)
                    def _(step):
                        act(edge_copy(n, after(me, step, blocks), t, kind, me))

    def start_edge(n):
        each_edge(n, lambda copy: copy.start())

    def finish_edge(n):
        each_edge(n, lambda copy: copy.wait_send())

    def receive_edge(n):
        for kind in (0, 1):
            own = 0 if kind else last
            for t in range(subs):
                if t not in targets(n, kind):
                    continue
                first = 1 if t == own else 0

                @pl.when(sub == t)
                def _():
                    @pl.loop(first, blocks)
                    def _(step):
                        source = after(me, step, blocks)
                        edge_copy(n, source, t, kind, source).wait_recv()

    def start_copy(source, target):
        return pltpu.make_async_remote_copy(
            src_ref=starts.at[source], dst_ref=starts.at[source], send_sem=us_sem.at[target],
            recv_sem=ur_sem.at[source], device_id=(me, target), device_id_type=MESH)

    def prefix_copy(n, source, target):
        return pltpu.make_async_remote_copy(
            src_ref=prefix.at[n, source], dst_ref=prefix.at[n, source], send_sem=ps_sem.at[n, target],
            recv_sem=pr_sem.at[n, source], device_id=(me, target), device_id_type=MESH)

    def splat(level, matrix):
        return jnp.stack([
            jnp.stack([jnp.full((SUBLANES, LANES), couple[a, b, level, matrix], jnp.float32) for a in range(NV)])
            for b in range(NV)
        ])

    identity = jnp.stack([
        jnp.stack([jnp.full((SUBLANES, LANES), 1.0 if a == b else 0.0, jnp.float32) for a in range(NV)])
        for b in range(NV)
    ])

    def prepare(level, store):
        for matrix in range(7):
            store[RAW + matrix] = splat(level, matrix)
        store[INV] = identity

        @pl.loop(0, 6)
        def _(repeat):
            approx = store[INV]
            store[INV] = product(approx, 2.0 * identity - product(store[RAW], approx))

        @pl.loop(0, 6)
        def _(matrix):
            store[IM + matrix] = product(store[INV], store[RAW + 1 + matrix])

    def powers(base, second, sixteenth, count):
        coef[second] = product(coef[base], coef[base])
        coef[second + 1] = product(coef[second], coef[second])
        coef[second + 2] = product(coef[second + 1], coef[second + 1])
        coef[sixteenth] = product(coef[second + 2], coef[second + 2])
        run = jnp.where((count & 1) != 0, coef[base], identity)
        for bit, index in ((2, second), (4, second + 1), (8, second + 2)):
            run = product(jnp.where((count & bit) != 0, coef[index], identity), run)
        coef[second + 3] = run


    def combined():
        seventh = product(coef[B4], product(coef[B2], coef[BWD]))

        @pl.loop(0, NV)
        def _(n):
            middle = jnp.where(n == 0, identity, coef[jnp.maximum(IM + n - 1, IM)])
            total = product(middle, coef[FWD])
            for back, ahead in ((BWD, FWD), (B2, F2), (B4, F4)):
                total = total + product(coef[back], product(total, coef[ahead]))
            coef[G0 + n] = jnp.where(place < subs, total, product(seventh, middle))

    def apply(index, values, height=SUBLANES):
        total = None
        for b in range(NV):
            term = coef[index, b][:, None, :height] * values[b][None]
            total = term if total is None else total + term
        return total

    in_low = lane < BJ
    in_high = lane >= LANES - BJ
    j_first = (lane & (BJ - 1)) == 0
    j_final = (lane & (BJ - 1)) == BJ - 1

    def lateral(values, base):
        zero = jnp.zeros_like(values[:, :1])
        turned = pltpu.roll(values, BJ, 3)
        total = apply(base, jnp.where(in_low, jnp.concatenate([zero, turned[:, :-1]], axis=1), turned))
        turned = pltpu.roll(values, LANES - BJ, 3)
        total = total + apply(base + 1, jnp.where(in_high, jnp.concatenate([turned[:, 1:], zero], axis=1), turned))
        total = total + apply(base + 2, jnp.where(j_first, 0.0, pltpu.roll(values, 1, 3)))
        return total + apply(base + 3, jnp.where(j_final, 0.0, pltpu.roll(values, LANES - 1, 3)))

    def scan(values, indices, reverse, length=planes):
        by = 1
        for index in indices:
            if reverse:
                shifted = jnp.where(place < length - by, pltpu.roll(values, SUBLANES - by, 2), 0.0)
            else:
                shifted = jnp.where((place >= by) & (place < length), pltpu.roll(values, by, 2), 0.0)
            values = values + apply(index, shifted)
            by *= 2
        return values

    def local(n):
        yf[...] = scan(sf[...], (FWD, F2, F4), False)
        tf[...] = cg[...] + lateral(yf[...], IM) + (yf[...] - sf[...])
        part = scan(tf[...], (BWD, B2, B4), True)
        prefix[n, sub, 0] = yf[:, :, planes - 1:planes, :]
        prefix[n, sub, 1] = part[:, :, 0:1, :]

    def send_prefix(n):
        for target in range(subs):
            @pl.when(sub != target)
            def _():
                prefix_copy(n, sub, target).start()

    def finish_prefix(n):
        for target in range(subs):
            @pl.when(sub != target)
            def _():
                prefix_copy(n, sub, target).wait_send()

    fetch[0].wait()
    starts[sub] = solution[:, :, 0:1, :]
    stage_edge(0, solution)
    pl.semaphore_wait(pltpu.get_barrier_semaphore(), count_all - 1)
    start_edge(0)
    for target in range(subs):
        @pl.when((sub > 0) & (sub != target))
        def _():
            start_copy(sub, target).start()
    fetch[2].wait()
    prepare(0, coef)
    powers(FWD, F2, F16, place + 1)
    powers(BWD, B2, B16, planes - place)
    fetch[1].wait()
    cg[...] = apply(INV, right_side[...])
    upper = jnp.where(place == planes - 1, 0.0, pltpu.roll(solution[...], planes - 1, 2))
    sf[...] = cg[...] + lateral(solution[...], IM) + apply(BWD, upper)
    local(0)
    send_prefix(0)
    combined()

    def prepare_coarse():
        for number, store in ((1, coef_one), (2, coef_two)):
            prepare(number, store)
            width = BJ >> number
            cells = rows * LANES >> (2 * number)
            inside = lane < cells
            masks = ((lane >= width) & inside, lane < cells - width,
                     ((lane & (width - 1)) != 0) & inside, ((lane & (width - 1)) != width - 1) & inside)
            for shift, mask in enumerate(masks):
                for base in (RAW + 1, IM):
                    store[base + shift] = jnp.where(mask, store[base + shift], 0.0)

    for n in range(SWEEPS_FINE):
        for source in range(subs):
            @pl.when(sub != source)
            def _():
                if n == 0 and source > 0:
                    start_copy(source, sub).wait_recv()
                prefix_copy(n, source, sub).wait_recv()
        receive_edge(n)
        below = edge_w[n][down[me]]
        above = edge_a[n][partner[me]]
        missing = above if n == 0 else above - old_above[...]
        ahead = jnp.where(place == subs + last, missing, 0.0)
        if n == 0:
            for s in range(last):
                ahead = jnp.where(place == subs + s, starts[s + 1], ahead)
        old_above[...] = above
        ahead = apply(BWD, ahead)
        enter = jnp.where(place == 0, below, 0.0)
        final = jnp.zeros_like(enter)
        for s in range(subs):
            if s < last:
                enter = jnp.where(place == s + 1, prefix[n, s, 0], enter)
            if s > 0:
                final = jnp.where(place == s, prefix[n, s, 1], final)
        moved = pltpu.roll(ahead, SUBLANES + 1 - subs, 2)
        enter = enter + jnp.where((place > 0) & (place < subs), moved, 0.0)
        enter = scan(enter, (F8, F16), False, subs)
        both = enter + ahead
        sides = lateral(both, G1)
        final = final + apply(G0, enter) + sides + pltpu.roll(sides, SUBLANES - subs, 2)
        final = jnp.where(place < last, pltpu.roll(final, SUBLANES - 1, 2), jnp.where(place == last, above, 0.0))
        final = scan(final, (B8, B16), True, subs)
        wide[0] = both
        wide[1] = final
        enter = wide[0, :, :, pl.ds(sub, 1), :]
        extra = jnp.where(place == planes - 1, wide[0, :, :, pl.ds(subs + sub, 1), :], 0.0)
        y = yf[...] + apply(FP, enter) + extra
        yf[...] = y
        tf[...] = cg[...] + lateral(y, IM) + (y - (sf[...] + extra))
        zf[...] = scan(tf[...], (BWD, B2, B4), True) + apply(BP, wide[1, :, :, pl.ds(sub, 1), :])
        if n + 1 < SWEEPS_FINE:
            stage_edge(n + 1, zf)
            start_edge(n + 1)
            sf[...] = cg[...] + lateral(zf[...], IM) + (zf[...] - tf[...])
            local(n + 1)
            send_prefix(n + 1)
            if n == 0:
                prepare_coarse()
                finish_edge(0)
                finish_prefix(0)
                for target in range(subs):
                    @pl.when((sub > 0) & (sub != target))
                    def _():
                        start_copy(sub, target).wait_send()

    change = zf[...] - yf[...]
    lower = jnp.where(place == 0, -wide[0, :, :, pl.ds(sub, 1), :], pltpu.roll(change, 1, 2))
    upper = jnp.where((place == planes - 1) & is_high, -old_above[...], 0.0)
    sf[...] = lateral(change, RAW + 1) + apply(RAW + 5, lower) + apply(RAW + 6, upper)

    height = rows * LANES
    r_row = lax.broadcasted_iota(jnp.int32, (height, LANES), 0)
    r_col = lax.broadcasted_iota(jnp.int32, (height, LANES), 1)
    half = BJ // 2
    share = ((((r_row >> 5) * half) + ((r_row & (BJ - 1)) >> 1)) == r_col).astype(jnp.float32)
    reduced = None
    for r in range(rows):
        both = jnp.concatenate([sf[:, r].reshape(NV * SUBLANES, LANES), zf[:, r].reshape(NV * SUBLANES, LANES)], axis=0)
        term = chosen(both, share[r * LANES:(r + 1) * LANES])
        reduced = term if reduced is None else reduced + term
    count = NV * planes // 2
    rsum[...] = reduced * 0.125
    gathered[sub, me, 0:count, :] = rsum[pl.ds(0, count, stride=2), :] + rsum[pl.ds(1, count, stride=2), :]
    tail = gathered.shape[2] - count - 2 * NV
    gathered[sub, me, count:count + NV, :] = rsum[pl.ds(NV * planes + planes - 1, NV, stride=planes), :]
    gathered[sub, me, count + NV:count + 2 * NV, :] = rsum[pl.ds(NV * planes, NV, stride=planes), :]
    gathered[sub, me, count + 2 * NV:, :] = jnp.zeros((tail, LANES), jnp.float32)

    def spread_copy(source, target):
        return pltpu.make_async_remote_copy(
            src_ref=gathered.at[sub, source], dst_ref=gathered.at[sub, source], send_sem=gs_sem.at[target],
            recv_sem=gr_sem.at[source], device_id=(target, sub), device_id_type=MESH)

    @pl.loop(1, blocks)
    def _(step):
        spread_copy(me, after(me, step, blocks)).start()

    def across_copy(source, block, target):
        return pltpu.make_async_remote_copy(
            src_ref=gathered.at[source, block], dst_ref=gathered.at[source, block],
            send_sem=es_sem.at[target, block], recv_sem=er_sem.at[source, block],
            device_id=(me, target), device_id_type=MESH)

    for step in range(1, subs):
        across_copy(sub, me, after(sub, step, subs)).start()

    stage_edge(SWEEPS_FINE, zf)
    start_edge(SWEEPS_FINE)
    low_recv[0] = zf[:, :, planes - 1:planes, :]

    def halo_copy(target):
        return pltpu.make_async_remote_copy(
            src_ref=low_recv.at[0], dst_ref=low_recv.at[1], send_sem=hs_sem.at[0], recv_sem=hr_sem.at[0],
            device_id=(me, target), device_id_type=MESH)

    @pl.when(jnp.logical_not(is_high))
    def _():
        halo_copy(sub + 1).start()

    @pl.loop(1, blocks)
    def _(step):
        source = after(me, step, blocks)
        spread_copy(source, source).wait_recv()
        for turn in range(1, subs):
            across_copy(sub, source, after(sub, turn, subs)).start()

    for n in range(1, SWEEPS_FINE):
        finish_edge(n)
        finish_prefix(n)

    @pl.loop(1, blocks)
    def _(step):
        spread_copy(me, after(me, step, blocks)).wait_send()

    receive_edge(SWEEPS_FINE)

    @pl.when(is_low)
    def _():
        low_recv[1] = edge_w[SWEEPS_FINE][down[me]]

    @pl.when(is_high)
    def _():
        fresh = apply(RAW + 6, edge_a[SWEEPS_FINE][partner[me]], 1)
        sf[:, :, planes - 1:planes, :] = sf[:, :, planes - 1:planes, :] + fresh

    @pl.when(jnp.logical_not(is_low))
    def _():
        halo_copy(sub).wait_recv()

    sf[:, :, 0:1, :] = sf[:, :, 0:1, :] + apply(RAW + 5, low_recv[1], 1)
    residual = sf[...]
    squares_recv[here] = jnp.sum((residual * residual).reshape(NV * rows * SUBLANES, LANES), axis=0, keepdims=True)

    def norm_copy(source, b, t):
        return pltpu.make_async_remote_copy(
            src_ref=squares_recv.at[source], dst_ref=squares_recv.at[source], send_sem=ns_sem.at[b * subs + t],
            recv_sem=nr_sem.at[source], device_id=(b, t), device_id_type=MESH)

    everyone(lambda b, t: norm_copy(here, b, t).start())

    @pl.loop(0, blocks)
    def _(block):
        for turn in range(1, subs):
            source = after(sub, turn, subs)
            across_copy(source, block, source).wait_recv()

    def use(store, index, values):
        cut = values.reshape(NV, -1, SUBLANES, LANES)
        terms = [store[index, b][:, None] * cut[b][None] for b in range(NV)]
        out = (terms[0] + terms[1]) + (terms[2] + terms[3]) + terms[4]
        return out.reshape(values.shape)

    slot = lax.broadcasted_iota(jnp.int32, (blocks, 1), 0)

    def codes(source):
        out = jnp.zeros((blocks, 1), jnp.int32)
        for n in range(blocks):
            out = jnp.where(slot == n, source(n), out)
        return out

    code_below = codes(lambda n: orient[down[n]])
    code_above = codes(lambda n: orient[n])

    def turned(values, code, cells, width):
        high = jnp.where((code & 1) != 0, cells - width, 0)
        return permute(values, lane ^ high ^ jnp.where(code >= 2, width - 1, 0))

    local_planes = planes // 2
    cells_one = rows * LANES // 4

    def edge_rows(s, pick, first):
        return jnp.stack([
            jnp.concatenate([gathered[s, pl.ds(pick(n), 1), first + a, :] for n in range(blocks)], axis=0)
            for a in range(NV)])

    under = turned(edge_rows(last, lambda n: down[n], count), code_below, cells_one, BJ // 2)
    over = turned(edge_rows(0, lambda n: partner[n], count + NV), code_above, cells_one, BJ // 2)
    for s in range(subs):
        if s > 0:
            under = jnp.stack([gathered[s - 1, :, count + a, :] for a in range(NV)])
        under = use(coef, RAW + 5, under)
        for k in range(local_planes):
            value = jnp.stack([gathered[s, :, a * local_planes + k, :] for a in range(NV)])
            if k == 0:
                value = value + under
            if s == last and k == local_planes - 1:
                value = value + use(coef, RAW + 6, over)
            field_f[:, s * local_planes + k] = value

    def root_mean(value, entries):
        return jnp.sqrt(jnp.sum(value, axis=1, keepdims=True) / jnp.float32(entries))

    size = NV * blocks * subs * planes * rows * LANES

    def level(store, cells, width, g, c, p, v, y, sweeps):
        depth = g.shape[1]
        chunk = max(1, 4 * SUBLANES // blocks)
        steps = depth // chunk

        def repeat(body, start, number):
            return lax.fori_loop(0, number, body, start, unroll=blocks <= SUBLANES)

        def sides(values, base):
            axis = values.ndim - 1
            out = use(store, base, pltpu.roll(values, width, axis))
            out = out + use(store, base + 1, pltpu.roll(values, LANES - width, axis))
            out = out + use(store, base + 2, pltpu.roll(values, 1, axis))
            return out + use(store, base + 3, pltpu.roll(values, LANES - 1, axis))

        def interfaces():
            below = jnp.concatenate([v[:, depth - 1, pl.ds(down[n], 1), :] for n in range(blocks)], axis=1)
            above = jnp.concatenate([v[:, 0, pl.ds(partner[n], 1), :] for n in range(blocks)], axis=1)
            return turned(below, code_below, cells, width), turned(above, code_above, cells, width)

        def centre(step, carry):
            at = pl.ds(step * chunk, chunk)
            c[:, at] = use(store, INV, g[:, at])
            return carry

        repeat(centre, 0, steps)
        nothing = jnp.zeros((NV, blocks, LANES), jnp.float32)
        below, above = nothing, nothing
        for n in range(sweeps):
            if n > 0:
                below, above = interfaces()
                p[:, depth - 1] = use(store, BWD, above)

            def forward(step, previous):
                at = pl.ds(step * chunk, chunk)
                s = c[:, at]
                if n > 0:
                    s = s + sides(v[:, at], IM) + p[:, at]
                made = []
                for u in range(chunk):
                    behind = use(store, FWD, previous)
                    previous = s[:, u] + behind
                    made.append((previous, behind))
                for u, (now, behind) in enumerate(made):
                    y[:, step * chunk + u] = now
                    p[:, step * chunk + u] = behind
                return previous

            repeat(forward, below, steps)

            def backward(step, following):
                start = depth - chunk - step * chunk
                at = pl.ds(start, chunk)
                t = c[:, at] + sides(y[:, at], IM) + p[:, at]
                made = []
                for u in range(chunk - 1, -1, -1):
                    ahead = use(store, BWD, following)
                    following = t[:, u] + ahead
                    made.append((u, following, ahead))
                for u, now, ahead in made:
                    v[:, start + u] = now
                    p[:, start + u] = ahead
                return following

            repeat(backward, above, steps)

        new_below, new_above = interfaces()
        top = use(store, RAW + 6, new_above - above)

        def remain(step, carry, final=False):
            squares, previous = carry
            at = pl.ds(step * chunk, chunk)
            change = v[:, at] - y[:, at]
            shifted = jnp.stack([previous] + [change[:, u] for u in range(chunk - 1)], axis=1)
            out = sides(change, RAW + 1) + use(store, RAW + 5, shifted)
            if final:
                out = jnp.stack([out[:, u] for u in range(chunk - 1)] + [out[:, chunk - 1] + top], axis=1)
            c[:, at] = out
            return squares + jnp.sum(out * out, axis=1), change[:, chunk - 1]

        carry = repeat(remain, (nothing, new_below - below), steps - 1)
        squares, _ = remain(steps - 1, carry, True)
        return jnp.sum(squares.reshape(NV * blocks, LANES), axis=0, keepdims=True)

    depth_one = field_f.shape[1]
    total = level(coef_one, cells_one, BJ // 2, field_f, field_c, field_p, field_v, field_y, SWEEPS_MID)
    norms[1:2, :] = jnp.broadcast_to(root_mean(total, size // 8), (1, LANES))

    s_row = lax.broadcasted_iota(jnp.int32, (LANES, LANES), 0)
    s_col = lax.broadcasted_iota(jnp.int32, (LANES, LANES), 1)
    fold = ((((s_row >> 4) * (BJ // 4)) + ((s_row & (BJ // 2 - 1)) >> 1)) == s_col).astype(jnp.float32)
    depth_two = depth_one // 2

    pairs = jnp.stack([field_c[:, 2 * k] + field_c[:, 2 * k + 1] for k in range(depth_two)], axis=1)
    two_f[...] = chosen(pairs.reshape(-1, LANES) * 0.125, fold).reshape(two_f.shape)

    total = level(coef_two, cells_one // 4, BJ // 4, two_f, two_c, two_p, two_v, two_y, SWEEPS_COARSE)
    norms[2:3, :] = jnp.broadcast_to(root_mean(total, size // 64), (1, LANES))

    unfold = ((((s_col >> 4) * (BJ // 4)) + ((s_col & (BJ // 2 - 1)) >> 1)) == s_row).astype(jnp.float32)
    coarse_planes = local_planes // 2
    for which, block in enumerate((me, held[0])):
        for a in range(NV):
            for k in range(coarse_planes):
                row = (which * NV + a) * coarse_planes + k
                rsum[row:row + 1, :] = two_v[a, sub * coarse_planes + k, pl.ds(block, 1), :]
    for a in range(NV):
        for k in range(coarse_planes):
            out_two[a, pl.ds(k, 1), :] = two_v[a, sub * coarse_planes + k, pl.ds(held[1], 1), :]
    filled = -(-2 * NV * coarse_planes // SUBLANES) * SUBLANES
    rsum[0:filled, :] = chosen(rsum[0:filled, :], unfold)
    for a in range(NV):
        for k in range(local_planes):
            at = sub * local_planes + k
            mine = a * coarse_planes + k // 2
            row = field_v[a, at, pl.ds(me, 1), :] + rsum[mine:mine + 1, :]
            spread[pl.ds(a * planes + 2 * k, 2), :] = jnp.broadcast_to(row, (2, LANES))
            mine = mine + NV * coarse_planes
            out_one[a, pl.ds(k, 1), :] = field_v[a, at, pl.ds(held[0], 1), :] + rsum[mine:mine + 1, :]

    for r in range(rows):
        grow = ((((s_col + r * LANES) >> 5) * half) + ((s_col & (BJ - 1)) >> 1) == s_row).astype(jnp.float32)
        corrected[:, r] = zf[:, r] + chosen(spread[...], grow).reshape(NV, SUBLANES, LANES)

    @pl.loop(0, blocks)
    def _(block):
        for turn in range(1, subs):
            across_copy(sub, block, after(sub, turn, subs)).wait_send()

    finish_edge(SWEEPS_FINE)

    @pl.when(jnp.logical_not(is_high))
    def _():
        halo_copy(sub + 1).wait_send()

    everyone(lambda b, t: norm_copy(b * subs + t, b, t).wait_recv())
    total = jnp.sum(squares_recv[...].reshape(count_all, LANES), axis=0, keepdims=True)
    norms[0:1, :] = jnp.broadcast_to(root_mean(total, size), (1, LANES))
    everyone(lambda b, t: norm_copy(here, b, t).wait_send())


def finish(corrected, one, two, norms, out, out_one, out_two, out_norms):
    for r in range(corrected.shape[1]):
        out[:, 0, :, r * LANES:(r + 1) * LANES] = corrected[:, r]
    out_one[:, 0] = one[...]
    out_two[:, 0] = two[:, :, :out_two.shape[3]]
    for n in range(3):
        out_norms[n] = jnp.max(norms[n:n + 1, :])


def shards(solution, right_side, couple, partner, orient, owner_one, owner_two):
    blocks = lax.axis_size("blk")
    subs = lax.axis_size("sub")
    planes, cells = solution.shape[2:]
    rows = cells // LANES
    tall = planes * subs

    def tiled(x):
        return x.reshape(NV, planes, rows, LANES).transpose(0, 2, 1, 3)

    vmem = pl.BlockSpec(memory_space=pltpu.VMEM)
    smem = pl.BlockSpec(memory_space=pltpu.SMEM)
    hbm = pl.BlockSpec(memory_space=pl.ANY)
    f32 = jnp.float32
    fine = pltpu.VMEM((NV, rows, planes, LANES), f32)
    plane = (NV, rows, 1, LANES)
    mid = pltpu.VMEM((NV, tall // 2, blocks, LANES), f32)
    low = pltpu.VMEM((NV, tall // 4, blocks, LANES), f32)
    matrix = (NV, NV, SUBLANES, LANES)
    payload = -(-(NV * planes // 2 + 2 * NV) // SUBLANES) * SUBLANES
    dma = pltpu.SemaphoreType.DMA
    edges = SWEEPS_FINE + 1
    everyone = blocks * subs
    couple = couple.transpose(2, 3, 0, 1)
    results = pl.pallas_call(
        functools.partial(kernel, (blocks, subs)),
        name="vcycle",
        out_shape=(
            pltpu.VMEM((NV, rows, planes, LANES), f32),
            pltpu.VMEM((NV, planes // 2, LANES), f32),
            pltpu.VMEM((NV, planes // 4, LANES), f32),
            pltpu.VMEM((3, LANES), f32),
        ),
        in_specs=[hbm] * 7,
        out_specs=(vmem, vmem, vmem, vmem),
        scratch_shapes=[
            pltpu.VMEM((29,) + matrix, f32), pltpu.VMEM((14,) + matrix, f32), pltpu.VMEM((14,) + matrix, f32),
            fine, fine, fine, fine, fine, pltpu.VMEM((2, NV, rows, planes, LANES), f32), pltpu.VMEM(plane, f32),
            pltpu.VMEM((edges,) + plane, f32),
            *[pltpu.VMEM((blocks,) + plane, f32)] * (2 * edges),
            pltpu.VMEM((subs,) + plane, f32),
            pltpu.VMEM((SWEEPS_FINE, subs, 2) + plane, f32),
            pltpu.VMEM((subs, blocks, payload, LANES), f32),
            pltpu.VMEM((2 * NV * planes, LANES), f32),
            pltpu.VMEM((2,) + plane, f32),
            pltpu.VMEM((everyone, 1, LANES), f32),
            pltpu.SMEM((blocks,), jnp.int32),
            mid, mid, mid, mid, mid, low, low, low, low, low,
            pltpu.VMEM((NV * planes, LANES), f32),
            dma((edges, blocks, subs)), dma((edges, blocks)), dma((edges, blocks)),
            dma((subs,)), dma((subs,)),
            dma((SWEEPS_FINE, subs)), dma((SWEEPS_FINE, subs)),
            dma((blocks,)), dma((blocks,)), dma((subs, blocks)), dma((subs, blocks)),
            dma((1,)), dma((1,)), dma((everyone,)), dma((everyone,)),
            fine, fine, pltpu.SMEM(couple.shape, f32), *[pltpu.SMEM((blocks,), jnp.int32)] * 4, dma((7,)),
        ],
        compiler_params=pltpu.CompilerParams(collective_id=0, has_side_effects=True, vmem_limit_bytes=60 * 1024 * 1024),
    )(tiled(solution), tiled(right_side), couple, partner, orient, owner_one, owner_two)
    return pl.pallas_call(
        finish,
        name="finish",
        out_shape=(
            jax.ShapeDtypeStruct((NV, 1, planes, cells), f32),
            jax.ShapeDtypeStruct((NV, 1, planes // 2, cells // 4), f32),
            jax.ShapeDtypeStruct((NV, 1, planes // 4, cells // 16), f32),
            jax.ShapeDtypeStruct((3,), f32),
        ),
        in_specs=[vmem] * 4,
        out_specs=(vmem, vmem, vmem, smem),
    )(*[pltpu.with_memory_space_constraint(x, pltpu.VMEM) for x in results])


def solution(mesh):
    split = P(None, "blk", "sub", None)
    return jax.shard_map(
        shards,
        mesh=mesh,
        in_specs=(split, split, P(), P(), P(), P(), P()),
        out_specs=(split, split, split, P()),
        check_vma=False,
    )
```

```python
import functools

import jax
import jax.numpy as jnp
from jax import lax
from jax.experimental import pallas as pl
from jax.experimental.pallas import tpu as pltpu
from jax.sharding import PartitionSpec as P

BI = 32
BJ = 16
SWEEPS_FINE = 2
SWEEPS_MID = 2
SWEEPS_COARSE = 4
LANES = 128
SUBLANES = 8
NV = 5
MESH = pl.DeviceIdType.MESH

RAW = 0
INV, IM, IP, JM, JP, FWD, BWD = 7, 8, 9, 10, 11, 12, 13
F2, F4, F8, FP, B2, B4, B8, BP = 14, 15, 16, 17, 18, 19, 20, 21
F16, B16, G0, G1 = 22, 23, 24, 25


def product(left, right):
    total = left[0][None] * right[:, 0][:, None]
    for b in range(1, NV):
        total = total + left[b][None] * right[:, b][:, None]
    return total


def permute(values, places):
    flat = values.reshape(-1, LANES)
    index = jnp.broadcast_to(places, values.shape).reshape(-1, LANES)
    return jnp.take_along_axis(flat, index, axis=1, mode="promise_in_bounds").reshape(values.shape)


def halves(values):
    high = values.astype(jnp.bfloat16)
    return high, (values - high.astype(jnp.float32)).astype(jnp.bfloat16)


def chosen(values, selection):
    high, low = halves(values)
    picks = selection.astype(jnp.bfloat16)
    return (jnp.dot(high, picks, preferred_element_type=jnp.float32)
            + jnp.dot(low, picks, preferred_element_type=jnp.float32))


def kernel(
    sizes, solution_hbm, right_side_hbm, couple_hbm, partner_hbm, orient_hbm, owner_one_hbm, owner_two_hbm,
    corrected, out_one, out_two, norms,
    coef, coef_one, coef_two, cg, sf, yf, tf, zf, wide, old_above,
    xsend, *more,
):
    edges = SWEEPS_FINE + 1
    edge_w, edge_a, more = more[:edges], more[edges:2 * edges], more[2 * edges:]
    (
        starts, prefix, gathered, rsum, low_recv, squares_recv,
        down,
        field_f, field_c, field_p, field_v, field_y,
        two_f, two_c, two_p, two_v, two_y, spread,
        xs_sem, xw_sem, xa_sem, us_sem, ur_sem, ps_sem, pr_sem, gs_sem, gr_sem, es_sem, er_sem,
        hs_sem, hr_sem, ns_sem, nr_sem, solution, right_side, couple, partner, orient, owner_one, owner_two, in_sem,
        totals, ts_sem, tr_sem,
    ) = more
    blocks, subs = sizes
    me = lax.axis_index("blk")
    sub = lax.axis_index("sub")
    last = subs - 1
    is_low = sub == 0
    is_high = sub == last
    rows = solution.shape[1]
    planes = SUBLANES
    count_all = blocks * subs
    here = me * subs + sub
    fetch = [pltpu.make_async_copy(source, target, in_sem.at[n]) for n, (source, target) in enumerate(
        ((solution_hbm, solution), (right_side_hbm, right_side), (couple_hbm, couple), (partner_hbm, partner),
         (orient_hbm, orient), (owner_one_hbm, owner_one), (owner_two_hbm, owner_two)))]
    for copy in fetch:
        copy.start()

    def after(index, step, length):
        return jnp.where(index + step >= length, index + step - length, index + step)

    def peer(step):
        return after(me, step, blocks)

    def everyone(body):
        for turn in range(subs):
            part = after(sub, turn, subs)

            @pl.loop(0 if turn else 1, blocks)
            def _(step):
                body(after(me, step, blocks), part)

    everyone(lambda b, t: pl.semaphore_signal(
        pltpu.get_barrier_semaphore(), inc=1, device_id=(b, t), device_id_type=MESH))
    for copy in fetch[3:]:
        copy.wait()

    def found(mapping, value):
        return lax.fori_loop(0, blocks, lambda n, best: jnp.where(mapping[n] == value, n, best), 0,
                             unroll=blocks <= SUBLANES)

    source_below = found(partner, me)
    lane = lax.broadcasted_iota(jnp.int32, (1, LANES), 1)
    place = lax.broadcasted_iota(jnp.int32, (SUBLANES, LANES), 0)

    def edge_copy(n, b, t, kind, source):
        edge = edge_a if kind else edge_w
        return pltpu.make_async_remote_copy(
            src_ref=xsend.at[n], dst_ref=edge[n].at[source], send_sem=xs_sem.at[n, b, t],
            recv_sem=(xa_sem if kind else xw_sem).at[n, source], device_id=(b, t), device_id_type=MESH)

    def targets(n, kind):
        if n < SWEEPS_FINE:
            return (0, last) + tuple(range(1, last))
        return (last,) if kind else (0,)

    ends = ((1, is_low, 0, 0), (0, is_high, last, planes - 1))

    def stage_edge(n, ref):
        for kind, mine, own, at in ends:
            @pl.when(mine)
            def _():
                code = orient[source_below] if kind else orient[me]
                places = lane ^ jnp.where(code // 2 == 1, BJ - 1, 0) ^ jnp.where(code % 2 == 1, LANES - BJ, 0)
                moved = permute(ref[...], places)
                swapped = jnp.concatenate([moved[:, r:r + 1] for r in range(rows - 1, -1, -1)], axis=1)
                moved = jnp.where(code % 2 == 1, swapped, moved)[:, :, at:at + 1]
                xsend[n] = moved
                (edge_a if kind else edge_w)[n][me] = moved

    def each_edge(n, act):
        for kind, mine, own, at in ends:
            @pl.when(mine)
            def _():
                for t in targets(n, kind):
                    @pl.loop(1 if t == own else 0, blocks)
                    def _(step):
                        act(edge_copy(n, peer(step), t, kind, me))

    def start_edge(n):
        each_edge(n, lambda copy: copy.start())

    def finish_edge(n):
        each_edge(n, lambda copy: copy.wait_send())

    def receive_edge(n):
        for kind in (0, 1):
            own = 0 if kind else last
            for t in range(subs):
                if t not in targets(n, kind):
                    continue
                first = 1 if t == own else 0

                @pl.when(sub == t)
                def _():
                    @pl.loop(first, blocks)
                    def _(step):
                        source = after(me, step, blocks)
                        edge_copy(n, source, t, kind, source).wait_recv()

    def start_copy(source, target):
        return pltpu.make_async_remote_copy(
            src_ref=starts.at[source], dst_ref=starts.at[source], send_sem=us_sem.at[target],
            recv_sem=ur_sem.at[source], device_id=(me, target), device_id_type=MESH)

    def prefix_copy(n, source, target):
        return pltpu.make_async_remote_copy(
            src_ref=prefix.at[n, source], dst_ref=prefix.at[n, source], send_sem=ps_sem.at[n, target],
            recv_sem=pr_sem.at[n, source], device_id=(me, target), device_id_type=MESH)

    def splat(level, matrix):
        return jnp.stack([
            jnp.stack([jnp.full((SUBLANES, LANES), couple[a, b, level, matrix], jnp.float32) for a in range(NV)])
            for b in range(NV)
        ])

    identity = jnp.stack([
        jnp.stack([jnp.full((SUBLANES, LANES), 1.0 if a == b else 0.0, jnp.float32) for a in range(NV)])
        for b in range(NV)
    ])

    def prepare(level, store):
        for matrix in range(7):
            store[RAW + matrix] = splat(level, matrix)
        store[INV] = identity

        @pl.loop(0, 6)
        def _(repeat):
            approx = store[INV]
            store[INV] = product(approx, 2.0 * identity - product(store[RAW], approx))

        @pl.loop(0, 6)
        def _(matrix):
            store[IM + matrix] = product(store[INV], store[RAW + 1 + matrix])

    def powers(base, second, sixteenth, count):
        coef[second] = product(coef[base], coef[base])
        coef[second + 1] = product(coef[second], coef[second])
        coef[second + 2] = product(coef[second + 1], coef[second + 1])
        coef[sixteenth] = product(coef[second + 2], coef[second + 2])
        run = jnp.where((count & 1) != 0, coef[base], identity)
        for bit, index in ((2, second), (4, second + 1), (8, second + 2)):
            run = product(jnp.where((count & bit) != 0, coef[index], identity), run)
        coef[second + 3] = run


    def combined():
        seventh = product(coef[B4], product(coef[B2], coef[BWD]))

        @pl.loop(0, NV)
        def _(n):
            middle = jnp.where(n == 0, identity, coef[jnp.maximum(IM + n - 1, IM)])
            total = product(middle, coef[FWD])
            for back, ahead in ((BWD, FWD), (B2, F2), (B4, F4)):
                total = total + product(coef[back], product(total, coef[ahead]))
            coef[G0 + n] = jnp.where(place < subs, total, product(seventh, middle))

    def apply(index, values, height=SUBLANES):
        total = None
        for b in range(NV):
            term = coef[index, b][:, None, :height] * values[b][None]
            total = term if total is None else total + term
        return total

    in_low = lane < BJ
    in_high = lane >= LANES - BJ
    j_first = (lane & (BJ - 1)) == 0
    j_final = (lane & (BJ - 1)) == BJ - 1

    def lateral(values, base):
        zero = jnp.zeros_like(values[:, :1])
        turned = pltpu.roll(values, BJ, 3)
        total = apply(base, jnp.where(in_low, jnp.concatenate([zero, turned[:, :-1]], axis=1), turned))
        turned = pltpu.roll(values, LANES - BJ, 3)
        total = total + apply(base + 1, jnp.where(in_high, jnp.concatenate([turned[:, 1:], zero], axis=1), turned))
        total = total + apply(base + 2, jnp.where(j_first, 0.0, pltpu.roll(values, 1, 3)))
        return total + apply(base + 3, jnp.where(j_final, 0.0, pltpu.roll(values, LANES - 1, 3)))

    def scan(values, indices, reverse, length=planes):
        by = 1
        for index in indices:
            if reverse:
                shifted = jnp.where(place < length - by, pltpu.roll(values, SUBLANES - by, 2), 0.0)
            else:
                shifted = jnp.where((place >= by) & (place < length), pltpu.roll(values, by, 2), 0.0)
            values = values + apply(index, shifted)
            by *= 2
        return values

    def local(n):
        yf[...] = scan(sf[...], (FWD, F2, F4), False)
        tf[...] = cg[...] + lateral(yf[...], IM) + (yf[...] - sf[...])
        part = scan(tf[...], (BWD, B2, B4), True)
        prefix[n, sub, 0] = yf[:, :, planes - 1:planes, :]
        prefix[n, sub, 1] = part[:, :, 0:1, :]

    def send_prefix(n):
        for target in range(subs):
            @pl.when(sub != target)
            def _():
                prefix_copy(n, sub, target).start()

    def finish_prefix(n):
        for target in range(subs):
            @pl.when(sub != target)
            def _():
                prefix_copy(n, sub, target).wait_send()

    fetch[0].wait()
    starts[sub] = solution[:, :, 0:1, :]
    stage_edge(0, solution)
    pl.semaphore_wait(pltpu.get_barrier_semaphore(), count_all - 1)
    start_edge(0)
    for target in range(subs):
        @pl.when((sub > 0) & (sub != target))
        def _():
            start_copy(sub, target).start()
    fetch[2].wait()
    prepare(0, coef)
    powers(FWD, F2, F16, place + 1)
    powers(BWD, B2, B16, planes - place)
    fetch[1].wait()
    cg[...] = apply(INV, right_side[...])
    upper = jnp.where(place == planes - 1, 0.0, pltpu.roll(solution[...], planes - 1, 2))
    sf[...] = cg[...] + lateral(solution[...], IM) + apply(BWD, upper)
    local(0)
    send_prefix(0)
    combined()

    def prepare_coarse():
        for number, store in ((1, coef_one), (2, coef_two)):
            prepare(number, store)
            width = BJ >> number
            cells = rows * LANES >> (2 * number)
            inside = lane < cells
            masks = ((lane >= width) & inside, lane < cells - width,
                     ((lane & (width - 1)) != 0) & inside, ((lane & (width - 1)) != width - 1) & inside)
            for shift, mask in enumerate(masks):
                for base in (RAW + 1, IM):
                    store[base + shift] = jnp.where(mask, store[base + shift], 0.0)

    @pl.loop(0, blocks)
    def _(n):
        down[n] = found(partner, n)

    held = (found(owner_one, me), found(owner_two, me))

    for n in range(SWEEPS_FINE):
        for source in range(subs):
            @pl.when(sub != source)
            def _():
                if n == 0 and source > 0:
                    start_copy(source, sub).wait_recv()
                prefix_copy(n, source, sub).wait_recv()
        receive_edge(n)
        below = edge_w[n][source_below]
        above = edge_a[n][partner[me]]
        missing = above if n == 0 else above - old_above[...]
        ahead = jnp.where(place == subs + last, missing, 0.0)
        if n == 0:
            for s in range(last):
                ahead = jnp.where(place == subs + s, starts[s + 1], ahead)
        old_above[...] = above
        ahead = apply(BWD, ahead)
        enter = jnp.where(place == 0, below, 0.0)
        final = jnp.zeros_like(enter)
        for s in range(subs):
            if s < last:
                enter = jnp.where(place == s + 1, prefix[n, s, 0], enter)
            if s > 0:
                final = jnp.where(place == s, prefix[n, s, 1], final)
        moved = pltpu.roll(ahead, SUBLANES + 1 - subs, 2)
        enter = enter + jnp.where((place > 0) & (place < subs), moved, 0.0)
        enter = scan(enter, (F8, F16), False, subs)
        both = enter + ahead
        sides = lateral(both, G1)
        final = final + apply(G0, enter) + sides + pltpu.roll(sides, SUBLANES - subs, 2)
        final = jnp.where(place < last, pltpu.roll(final, SUBLANES - 1, 2), jnp.where(place == last, above, 0.0))
        final = scan(final, (B8, B16), True, subs)
        wide[0] = both
        wide[1] = final
        enter = wide[0, :, :, pl.ds(sub, 1), :]
        extra = jnp.where(place == planes - 1, wide[0, :, :, pl.ds(subs + sub, 1), :], 0.0)
        y = yf[...] + apply(FP, enter) + extra
        yf[...] = y
        tf[...] = cg[...] + lateral(y, IM) + (y - (sf[...] + extra))
        zf[...] = scan(tf[...], (BWD, B2, B4), True) + apply(BP, wide[1, :, :, pl.ds(sub, 1), :])
        if n + 1 < SWEEPS_FINE:
            stage_edge(n + 1, zf)
            start_edge(n + 1)
            sf[...] = cg[...] + lateral(zf[...], IM) + (zf[...] - tf[...])
            local(n + 1)
            send_prefix(n + 1)
            if n == 0:
                prepare_coarse()
                finish_edge(0)
                finish_prefix(0)
                for target in range(subs):
                    @pl.when((sub > 0) & (sub != target))
                    def _():
                        start_copy(sub, target).wait_send()

    change = zf[...] - yf[...]
    lower = jnp.where(place == 0, -wide[0, :, :, pl.ds(sub, 1), :], pltpu.roll(change, 1, 2))
    upper = jnp.where((place == planes - 1) & is_high, -old_above[...], 0.0)
    sf[...] = lateral(change, RAW + 1) + apply(RAW + 5, lower) + apply(RAW + 6, upper)

    height = rows * LANES
    r_row = lax.broadcasted_iota(jnp.int32, (height, LANES), 0)
    r_col = lax.broadcasted_iota(jnp.int32, (height, LANES), 1)
    half = BJ // 2
    share = ((((r_row >> 5) * half) + ((r_row & (BJ - 1)) >> 1)) == r_col).astype(jnp.float32)
    reduced = None
    for r in range(rows):
        both = jnp.concatenate([sf[:, r].reshape(NV * SUBLANES, LANES), zf[:, r].reshape(NV * SUBLANES, LANES)], axis=0)
        term = chosen(both, share[r * LANES:(r + 1) * LANES])
        reduced = term if reduced is None else reduced + term
    count = NV * planes // 2
    rsum[...] = reduced * 0.125
    gathered[sub, me, 0:count, :] = rsum[pl.ds(0, count, stride=2), :] + rsum[pl.ds(1, count, stride=2), :]
    gathered[sub, me, count:count + NV, :] = rsum[pl.ds(NV * planes + planes - 1, NV, stride=planes), :]
    gathered[sub, me, count + NV:count + 2 * NV, :] = rsum[pl.ds(NV * planes, NV, stride=planes), :]

    def spread_copy(source, target):
        return pltpu.make_async_remote_copy(
            src_ref=gathered.at[sub, source], dst_ref=gathered.at[sub, source], send_sem=gs_sem.at[target],
            recv_sem=gr_sem.at[source], device_id=(target, sub), device_id_type=MESH)

    @pl.loop(1, blocks)
    def _(step):
        spread_copy(me, peer(step)).start()

    def across_copy(source, block, target):
        return pltpu.make_async_remote_copy(
            src_ref=gathered.at[source, block], dst_ref=gathered.at[source, block],
            send_sem=es_sem.at[target, block], recv_sem=er_sem.at[source, block],
            device_id=(me, target), device_id_type=MESH)

    for step in range(1, subs):
        across_copy(sub, me, after(sub, step, subs)).start()

    stage_edge(SWEEPS_FINE, zf)
    start_edge(SWEEPS_FINE)
    low_recv[0] = zf[:, :, planes - 1:planes, :]

    def halo_copy(target):
        return pltpu.make_async_remote_copy(
            src_ref=low_recv.at[0], dst_ref=low_recv.at[1], send_sem=hs_sem.at[0], recv_sem=hr_sem.at[0],
            device_id=(me, target), device_id_type=MESH)

    @pl.when(jnp.logical_not(is_high))
    def _():
        halo_copy(sub + 1).start()

    @pl.loop(1, blocks)
    def _(step):
        source = after(me, step, blocks)
        spread_copy(source, source).wait_recv()
        for turn in range(1, subs):
            across_copy(sub, source, after(sub, turn, subs)).start()

    for n in range(1, SWEEPS_FINE):
        finish_edge(n)
        finish_prefix(n)

    @pl.loop(1, blocks)
    def _(step):
        spread_copy(me, after(me, step, blocks)).wait_send()

    receive_edge(SWEEPS_FINE)

    @pl.when(is_low)
    def _():
        low_recv[1] = edge_w[SWEEPS_FINE][source_below]

    @pl.when(is_high)
    def _():
        fresh = apply(RAW + 6, edge_a[SWEEPS_FINE][partner[me]], 1)
        sf[:, :, planes - 1:planes, :] = sf[:, :, planes - 1:planes, :] + fresh

    @pl.when(jnp.logical_not(is_low))
    def _():
        halo_copy(sub).wait_recv()

    sf[:, :, 0:1, :] = sf[:, :, 0:1, :] + apply(RAW + 5, low_recv[1], 1)
    residual = sf[...]
    squares_recv[me] = jnp.sum((residual * residual).reshape(NV * rows * SUBLANES, LANES), axis=0, keepdims=True)

    def norm_copy(source, target):
        return pltpu.make_async_remote_copy(
            src_ref=squares_recv.at[source], dst_ref=squares_recv.at[source], send_sem=ns_sem.at[target],
            recv_sem=nr_sem.at[source], device_id=(target, sub), device_id_type=MESH)

    def total_copy(source, target):
        return pltpu.make_async_remote_copy(
            src_ref=totals.at[source], dst_ref=totals.at[source], send_sem=ts_sem.at[target],
            recv_sem=tr_sem.at[source], device_id=(me, target), device_id_type=MESH)

    @pl.loop(1, blocks)
    def _(step):
        norm_copy(me, peer(step)).start()

    @pl.loop(0, blocks)
    def _(block):
        for turn in range(1, subs):
            source = after(sub, turn, subs)
            across_copy(source, block, source).wait_recv()

    def use(store, index, values):
        cut = values.reshape(NV, -1, SUBLANES, LANES)
        terms = [store[index, b][:, None] * cut[b][None] for b in range(NV)]
        out = (terms[0] + terms[1]) + (terms[2] + terms[3]) + terms[4]
        return out.reshape(values.shape)

    slot = lax.broadcasted_iota(jnp.int32, (blocks, 1), 0)

    def codes(source):
        out = jnp.zeros((blocks, 1), jnp.int32)
        for n in range(blocks):
            out = jnp.where(slot == n, source(n), out)
        return out

    code_below = codes(lambda n: orient[down[n]])
    code_above = codes(lambda n: orient[n])

    def turned(values, code, cells, width):
        high = jnp.where((code & 1) != 0, cells - width, 0)
        return permute(values, lane ^ high ^ jnp.where(code >= 2, width - 1, 0))

    local_planes = planes // 2
    cells_one = rows * LANES // 4

    def edge_rows(s, pick, first):
        return jnp.stack([
            jnp.concatenate([gathered[s, pl.ds(pick(n), 1), first + a, :] for n in range(blocks)], axis=0)
            for a in range(NV)])

    under = turned(edge_rows(last, lambda n: down[n], count), code_below, cells_one, BJ // 2)
    over = turned(edge_rows(0, lambda n: partner[n], count + NV), code_above, cells_one, BJ // 2)
    for s in range(subs):
        if s > 0:
            under = jnp.stack([gathered[s - 1, :, count + a, :] for a in range(NV)])
        under = use(coef, RAW + 5, under)
        for k in range(local_planes):
            value = jnp.stack([gathered[s, :, a * local_planes + k, :] for a in range(NV)])
            if k == 0:
                value = value + under
            if s == last and k == local_planes - 1:
                value = value + use(coef, RAW + 6, over)
            field_f[:, s * local_planes + k] = value

    def root_mean(value, entries):
        return jnp.sqrt(jnp.sum(value, axis=1, keepdims=True) / jnp.float32(entries))

    size = NV * blocks * subs * planes * rows * LANES

    def level(store, cells, width, g, c, p, v, y, sweeps):
        depth = g.shape[1]
        chunk = max(1, 4 * SUBLANES // blocks)
        steps = depth // chunk

        def repeat(body, start, number):
            return lax.fori_loop(0, number, body, start, unroll=blocks <= SUBLANES)

        def sides(values, base):
            axis = values.ndim - 1
            out = use(store, base, pltpu.roll(values, width, axis))
            out = out + use(store, base + 1, pltpu.roll(values, LANES - width, axis))
            out = out + use(store, base + 2, pltpu.roll(values, 1, axis))
            return out + use(store, base + 3, pltpu.roll(values, LANES - 1, axis))

        def interfaces():
            below = jnp.concatenate([v[:, depth - 1, pl.ds(down[n], 1), :] for n in range(blocks)], axis=1)
            above = jnp.concatenate([v[:, 0, pl.ds(partner[n], 1), :] for n in range(blocks)], axis=1)
            return turned(below, code_below, cells, width), turned(above, code_above, cells, width)

        def centre(step, carry):
            at = pl.ds(step * chunk, chunk)
            c[:, at] = use(store, INV, g[:, at])
            return carry

        repeat(centre, 0, steps)
        nothing = jnp.zeros((NV, blocks, LANES), jnp.float32)
        below, above = nothing, nothing
        for n in range(sweeps):
            if n > 0:
                below, above = interfaces()
                p[:, depth - 1] = use(store, BWD, above)

            def forward(step, previous):
                at = pl.ds(step * chunk, chunk)
                s = c[:, at]
                if n > 0:
                    s = s + sides(v[:, at], IM) + p[:, at]
                made = []
                for u in range(chunk):
                    behind = use(store, FWD, previous)
                    previous = s[:, u] + behind
                    made.append((previous, behind))
                for u, (now, behind) in enumerate(made):
                    y[:, step * chunk + u] = now
                    p[:, step * chunk + u] = behind
                return previous

            repeat(forward, below, steps)

            def backward(step, following):
                start = depth - chunk - step * chunk
                at = pl.ds(start, chunk)
                t = c[:, at] + sides(y[:, at], IM) + p[:, at]
                made = []
                for u in range(chunk - 1, -1, -1):
                    ahead = use(store, BWD, following)
                    following = t[:, u] + ahead
                    made.append((u, following, ahead))
                for u, now, ahead in made:
                    v[:, start + u] = now
                    p[:, start + u] = ahead
                return following

            repeat(backward, above, steps)

        new_below, new_above = interfaces()
        top = use(store, RAW + 6, new_above - above)

        def remain(step, carry, final=False):
            squares, previous = carry
            at = pl.ds(step * chunk, chunk)
            change = v[:, at] - y[:, at]
            shifted = jnp.stack([previous] + [change[:, u] for u in range(chunk - 1)], axis=1)
            out = sides(change, RAW + 1) + use(store, RAW + 5, shifted)
            if final:
                out = jnp.stack([out[:, u] for u in range(chunk - 1)] + [out[:, chunk - 1] + top], axis=1)
            c[:, at] = out
            return squares + jnp.sum(out * out, axis=1), change[:, chunk - 1]

        carry = repeat(remain, (nothing, new_below - below), steps - 1)
        squares, _ = remain(steps - 1, carry, True)
        return jnp.sum(squares.reshape(NV * blocks, LANES), axis=0, keepdims=True)

    depth_one = field_f.shape[1]
    total = level(coef_one, cells_one, BJ // 2, field_f, field_c, field_p, field_v, field_y, SWEEPS_MID)
    norms[1:2, :] = jnp.broadcast_to(root_mean(total, size // 8), (1, LANES))

    @pl.loop(1, blocks)
    def _(step):
        source = peer(step)
        norm_copy(source, source).wait_recv()

    totals[sub] = jnp.sum(squares_recv[...].reshape(blocks, LANES), axis=0, keepdims=True)
    for turn in range(1, subs):
        total_copy(sub, after(sub, turn, subs)).start()

    @pl.loop(1, blocks)
    def _(step):
        norm_copy(me, peer(step)).wait_send()

    s_row = lax.broadcasted_iota(jnp.int32, (LANES, LANES), 0)
    s_col = lax.broadcasted_iota(jnp.int32, (LANES, LANES), 1)
    fold = ((((s_row >> 4) * (BJ // 4)) + ((s_row & (BJ // 2 - 1)) >> 1)) == s_col).astype(jnp.float32)
    depth_two = depth_one // 2

    pairs = jnp.stack([field_c[:, 2 * k] + field_c[:, 2 * k + 1] for k in range(depth_two)], axis=1)
    two_f[...] = chosen(pairs.reshape(-1, LANES) * 0.125, fold).reshape(two_f.shape)

    total = level(coef_two, cells_one // 4, BJ // 4, two_f, two_c, two_p, two_v, two_y, SWEEPS_COARSE)
    norms[2:3, :] = jnp.broadcast_to(root_mean(total, size // 64), (1, LANES))

    unfold = ((((s_col >> 4) * (BJ // 4)) + ((s_col & (BJ // 2 - 1)) >> 1)) == s_row).astype(jnp.float32)
    coarse_planes = local_planes // 2
    for which, block in enumerate((me, held[0])):
        for a in range(NV):
            for k in range(coarse_planes):
                row = (which * NV + a) * coarse_planes + k
                rsum[row:row + 1, :] = two_v[a, sub * coarse_planes + k, pl.ds(block, 1), :]
    for a in range(NV):
        for k in range(coarse_planes):
            out_two[a, pl.ds(k, 1), :] = two_v[a, sub * coarse_planes + k, pl.ds(held[1], 1), :]
    filled = -(-2 * NV * coarse_planes // SUBLANES) * SUBLANES
    rsum[0:filled, :] = chosen(rsum[0:filled, :], unfold)
    for a in range(NV):
        for k in range(local_planes):
            at = sub * local_planes + k
            mine = a * coarse_planes + k // 2
            row = field_v[a, at, pl.ds(me, 1), :] + rsum[mine:mine + 1, :]
            spread[pl.ds(a * planes + 2 * k, 2), :] = jnp.broadcast_to(row, (2, LANES))
            mine = mine + NV * coarse_planes
            out_one[a, pl.ds(k, 1), :] = field_v[a, at, pl.ds(held[0], 1), :] + rsum[mine:mine + 1, :]

    for r in range(rows):
        grow = ((((s_col + r * LANES) >> 5) * half) + ((s_col & (BJ - 1)) >> 1) == s_row).astype(jnp.float32)
        corrected[:, r] = zf[:, r] + chosen(spread[...], grow).reshape(NV, SUBLANES, LANES)

    @pl.loop(0, blocks)
    def _(block):
        for turn in range(1, subs):
            across_copy(sub, block, after(sub, turn, subs)).wait_send()

    finish_edge(SWEEPS_FINE)

    @pl.when(jnp.logical_not(is_high))
    def _():
        halo_copy(sub + 1).wait_send()

    for turn in range(1, subs):
        source = after(sub, turn, subs)
        total_copy(source, source).wait_recv()
    total = jnp.sum(totals[...].reshape(subs, LANES), axis=0, keepdims=True)
    norms[0:1, :] = jnp.broadcast_to(root_mean(total, size), (1, LANES))
    for turn in range(1, subs):
        total_copy(sub, after(sub, turn, subs)).wait_send()


def finish(corrected, one, two, norms, out, out_one, out_two, out_norms):
    for r in range(corrected.shape[1]):
        out[:, 0, :, r * LANES:(r + 1) * LANES] = corrected[:, r]
    out_one[:, 0] = one[...]
    out_two[:, 0] = two[:, :, :out_two.shape[3]]
    for n in range(3):
        out_norms[n] = jnp.max(norms[n:n + 1, :])


def shards(solution, right_side, couple, partner, orient, owner_one, owner_two):
    blocks = lax.axis_size("blk")
    subs = lax.axis_size("sub")
    planes, cells = solution.shape[2:]
    rows = cells // LANES
    tall = planes * subs

    def tiled(x):
        return x.reshape(NV, planes, rows, LANES).transpose(0, 2, 1, 3)

    vmem = pl.BlockSpec(memory_space=pltpu.VMEM)
    smem = pl.BlockSpec(memory_space=pltpu.SMEM)
    hbm = pl.BlockSpec(memory_space=pl.ANY)
    f32 = jnp.float32
    fine = pltpu.VMEM((NV, rows, planes, LANES), f32)
    plane = (NV, rows, 1, LANES)
    mid = pltpu.VMEM((NV, tall // 2, blocks, LANES), f32)
    low = pltpu.VMEM((NV, tall // 4, blocks, LANES), f32)
    matrix = (NV, NV, SUBLANES, LANES)
    payload = NV * planes // 2 + 2 * NV
    dma = pltpu.SemaphoreType.DMA
    edges = SWEEPS_FINE + 1
    couple = couple.transpose(2, 3, 0, 1)
    results = pl.pallas_call(
        functools.partial(kernel, (blocks, subs)),
        name="vcycle",
        out_shape=(
            pltpu.VMEM((NV, rows, planes, LANES), f32),
            pltpu.VMEM((NV, planes // 2, LANES), f32),
            pltpu.VMEM((NV, planes // 4, LANES), f32),
            pltpu.VMEM((3, LANES), f32),
        ),
        in_specs=[hbm] * 7,
        out_specs=(vmem, vmem, vmem, vmem),
        scratch_shapes=[
            pltpu.VMEM((29,) + matrix, f32), pltpu.VMEM((14,) + matrix, f32), pltpu.VMEM((14,) + matrix, f32),
            fine, fine, fine, fine, fine, pltpu.VMEM((2, NV, rows, planes, LANES), f32), pltpu.VMEM(plane, f32),
            pltpu.VMEM((edges,) + plane, f32),
            *[pltpu.VMEM((blocks,) + plane, f32)] * (2 * edges),
            pltpu.VMEM((subs,) + plane, f32),
            pltpu.VMEM((SWEEPS_FINE, subs, 2) + plane, f32),
            pltpu.VMEM((subs, blocks, payload, LANES), f32),
            pltpu.VMEM((2 * NV * planes, LANES), f32),
            pltpu.VMEM((2,) + plane, f32),
            pltpu.VMEM((blocks, 1, LANES), f32),
            pltpu.SMEM((blocks,), jnp.int32),
            mid, mid, mid, mid, mid, low, low, low, low, low,
            pltpu.VMEM((NV * planes, LANES), f32),
            dma((edges, blocks, subs)), dma((edges, blocks)), dma((edges, blocks)),
            dma((subs,)), dma((subs,)),
            dma((SWEEPS_FINE, subs)), dma((SWEEPS_FINE, subs)),
            dma((blocks,)), dma((blocks,)), dma((subs, blocks)), dma((subs, blocks)),
            dma((1,)), dma((1,)), dma((blocks,)), dma((blocks,)),
            fine, fine, pltpu.SMEM(couple.shape, f32), *[pltpu.SMEM((blocks,), jnp.int32)] * 4, dma((7,)),
            pltpu.VMEM((subs, 1, LANES), f32), dma((subs,)), dma((subs,)),
        ],
        compiler_params=pltpu.CompilerParams(collective_id=0, has_side_effects=True, vmem_limit_bytes=60 * 1024 * 1024),
    )(tiled(solution), tiled(right_side), couple, partner, orient, owner_one, owner_two)
    return pl.pallas_call(
        finish,
        name="finish",
        out_shape=(
            jax.ShapeDtypeStruct((NV, 1, planes, cells), f32),
            jax.ShapeDtypeStruct((NV, 1, planes // 2, cells // 4), f32),
            jax.ShapeDtypeStruct((NV, 1, planes // 4, cells // 16), f32),
            jax.ShapeDtypeStruct((3,), f32),
        ),
        in_specs=[vmem] * 4,
        out_specs=(vmem, vmem, vmem, smem),
    )(*[pltpu.with_memory_space_constraint(x, pltpu.VMEM) for x in results])


def solution(mesh):
    split = P(None, "blk", "sub", None)
    return jax.shard_map(
        shards,
        mesh=mesh,
        in_specs=(split, split, P(), P(), P(), P(), P()),
        out_specs=(split, split, split, P()),
        check_vma=False,
    )
```

```python
import functools

import jax
import jax.numpy as jnp
from jax import lax
from jax.experimental import pallas as pl
from jax.experimental.pallas import tpu as pltpu
from jax.sharding import PartitionSpec as P

BI = 32
BJ = 16
SWEEPS_FINE = 2
SWEEPS_MID = 2
SWEEPS_COARSE = 4
LANES = 128
SUBLANES = 8
NV = 5
MESH = pl.DeviceIdType.MESH

RAW = 0
INV, IM, IP, JM, JP, FWD, BWD = 7, 8, 9, 10, 11, 12, 13
F2, F4, F8, FP, B2, B4, B8, BP = 14, 15, 16, 17, 18, 19, 20, 21
F16, B16, G0, G1 = 22, 23, 24, 25


def product(left, right):
    total = left[0][None] * right[:, 0][:, None]
    for b in range(1, NV):
        total = total + left[b][None] * right[:, b][:, None]
    return total


def permute(values, places):
    flat = values.reshape(-1, LANES)
    index = jnp.broadcast_to(places, values.shape).reshape(-1, LANES)
    return jnp.take_along_axis(flat, index, axis=1, mode="promise_in_bounds").reshape(values.shape)


def halves(values):
    high = values.astype(jnp.bfloat16)
    return high, (values - high.astype(jnp.float32)).astype(jnp.bfloat16)


def chosen(values, selection):
    high, low = halves(values)
    picks = selection.astype(jnp.bfloat16)
    return (jnp.dot(high, picks, preferred_element_type=jnp.float32)
            + jnp.dot(low, picks, preferred_element_type=jnp.float32))


def kernel(
    sizes, solution_hbm, right_side_hbm, couple_hbm, partner_hbm, orient_hbm, owner_one_hbm, owner_two_hbm,
    corrected, out_one, out_two, norms,
    coef, coef_one, coef_two, cg, sf, yf, tf, zf, wide, old_above,
    xsend, *more,
):
    edges = SWEEPS_FINE + 1
    edge_w, edge_a, more = more[:edges], more[edges:2 * edges], more[2 * edges:]
    (
        starts, prefix, gathered, rsum, low_recv, squares_recv,
        down,
        field_f, field_c, field_p, field_v, field_y,
        two_f, two_c, two_p, two_v, two_y, spread,
        xs_sem, xw_sem, xa_sem, us_sem, ur_sem, ps_sem, pr_sem, gs_sem, gr_sem, es_sem, er_sem,
        hs_sem, hr_sem, ns_sem, nr_sem, solution, right_side, couple, partner, orient, owner_one, owner_two, in_sem,
        totals, ts_sem, tr_sem,
    ) = more
    blocks, subs = sizes
    me = lax.axis_index("blk")
    sub = lax.axis_index("sub")
    last = subs - 1
    is_low = sub == 0
    is_high = sub == last
    rows = solution.shape[1]
    planes = SUBLANES
    count_all = blocks * subs
    here = me * subs + sub
    fetch = [pltpu.make_async_copy(source, target, in_sem.at[n]) for n, (source, target) in enumerate(
        ((solution_hbm, solution), (right_side_hbm, right_side), (couple_hbm, couple), (partner_hbm, partner),
         (orient_hbm, orient), (owner_one_hbm, owner_one), (owner_two_hbm, owner_two)))]
    for copy in fetch:
        copy.start()

    def after(index, step, length):
        return jnp.where(index + step >= length, index + step - length, index + step)

    def peer(step):
        return after(me, step, blocks)

    def everyone(body):
        for turn in range(subs):
            part = after(sub, turn, subs)

            @pl.loop(0 if turn else 1, blocks)
            def _(step):
                body(after(me, step, blocks), part)

    everyone(lambda b, t: pl.semaphore_signal(
        pltpu.get_barrier_semaphore(), inc=1, device_id=(b, t), device_id_type=MESH))
    for copy in fetch[3:]:
        copy.wait()

    def found(mapping, value):
        return lax.fori_loop(0, blocks, lambda n, best: jnp.where(mapping[n] == value, n, best), 0,
                             unroll=blocks <= SUBLANES)

    source_below = found(partner, me)
    lane = lax.broadcasted_iota(jnp.int32, (1, LANES), 1)
    place = lax.broadcasted_iota(jnp.int32, (SUBLANES, LANES), 0)

    def edge_copy(n, b, t, kind, source):
        edge = edge_a if kind else edge_w
        return pltpu.make_async_remote_copy(
            src_ref=xsend.at[n], dst_ref=edge[n].at[source], send_sem=xs_sem.at[n, b, t],
            recv_sem=(xa_sem if kind else xw_sem).at[n, source], device_id=(b, t), device_id_type=MESH)

    def targets(n, kind):
        if n < SWEEPS_FINE:
            return (0, last) + tuple(range(1, last))
        return (last,) if kind else (0,)

    ends = ((1, is_low, 0, 0), (0, is_high, last, planes - 1))

    def stage_edge(n, ref):
        for kind, mine, own, at in ends:
            @pl.when(mine)
            def _():
                code = orient[source_below] if kind else orient[me]
                places = lane ^ jnp.where(code // 2 == 1, BJ - 1, 0) ^ jnp.where(code % 2 == 1, LANES - BJ, 0)
                moved = permute(ref[...], places)
                swapped = jnp.concatenate([moved[:, r:r + 1] for r in range(rows - 1, -1, -1)], axis=1)
                moved = jnp.where(code % 2 == 1, swapped, moved)[:, :, at:at + 1]
                xsend[n] = moved
                (edge_a if kind else edge_w)[n][me] = moved

    def each_edge(n, act):
        for kind, mine, own, at in ends:
            @pl.when(mine)
            def _():
                for t in targets(n, kind):
                    @pl.loop(1 if t == own else 0, blocks)
                    def _(step):
                        act(edge_copy(n, peer(step), t, kind, me))

    def start_edge(n):
        each_edge(n, lambda copy: copy.start())

    def finish_edge(n):
        each_edge(n, lambda copy: copy.wait_send())

    def receive_edge(n):
        for kind in (0, 1):
            own = 0 if kind else last
            for t in range(subs):
                if t not in targets(n, kind):
                    continue
                first = 1 if t == own else 0

                @pl.when(sub == t)
                def _():
                    @pl.loop(first, blocks)
                    def _(step):
                        source = after(me, step, blocks)
                        edge_copy(n, source, t, kind, source).wait_recv()

    def start_copy(source, target):
        return pltpu.make_async_remote_copy(
            src_ref=starts.at[source], dst_ref=starts.at[source], send_sem=us_sem.at[target],
            recv_sem=ur_sem.at[source], device_id=(me, target), device_id_type=MESH)

    def prefix_copy(n, source, target):
        return pltpu.make_async_remote_copy(
            src_ref=prefix.at[n, source], dst_ref=prefix.at[n, source], send_sem=ps_sem.at[n, target],
            recv_sem=pr_sem.at[n, source], device_id=(me, target), device_id_type=MESH)

    def splat(level, matrix):
        return jnp.stack([
            jnp.stack([jnp.full((SUBLANES, LANES), couple[a, b, level, matrix], jnp.float32) for a in range(NV)])
            for b in range(NV)
        ])

    identity = jnp.stack([
        jnp.stack([jnp.full((SUBLANES, LANES), 1.0 if a == b else 0.0, jnp.float32) for a in range(NV)])
        for b in range(NV)
    ])

    def prepare(level, store):
        for matrix in range(7):
            store[RAW + matrix] = splat(level, matrix)
        store[INV] = identity

        @pl.loop(0, 6)
        def _(repeat):
            approx = store[INV]
            store[INV] = product(approx, 2.0 * identity - product(store[RAW], approx))

        @pl.loop(0, 6)
        def _(matrix):
            store[IM + matrix] = product(store[INV], store[RAW + 1 + matrix])

    def powers(base, second, sixteenth, count):
        coef[second] = product(coef[base], coef[base])
        coef[second + 1] = product(coef[second], coef[second])
        coef[second + 2] = product(coef[second + 1], coef[second + 1])
        coef[sixteenth] = product(coef[second + 2], coef[second + 2])
        run = jnp.where((count & 1) != 0, coef[base], identity)
        for bit, index in ((2, second), (4, second + 1), (8, second + 2)):
            run = product(jnp.where((count & bit) != 0, coef[index], identity), run)
        coef[second + 3] = run


    def combined():
        seventh = product(coef[B4], product(coef[B2], coef[BWD]))

        @pl.loop(0, NV)
        def _(n):
            middle = jnp.where(n == 0, identity, coef[jnp.maximum(IM + n - 1, IM)])
            total = product(middle, coef[FWD])
            for back, ahead in ((BWD, FWD), (B2, F2), (B4, F4)):
                total = total + product(coef[back], product(total, coef[ahead]))
            coef[G0 + n] = jnp.where(place < subs, total, product(seventh, middle))

    def apply(index, values, height=SUBLANES):
        total = None
        for b in range(NV):
            term = coef[index, b][:, None, :height] * values[b][None]
            total = term if total is None else total + term
        return total

    in_low = lane < BJ
    in_high = lane >= LANES - BJ
    j_first = (lane & (BJ - 1)) == 0
    j_final = (lane & (BJ - 1)) == BJ - 1

    def lateral(values, base):
        zero = jnp.zeros_like(values[:, :1])
        turned = pltpu.roll(values, BJ, 3)
        total = apply(base, jnp.where(in_low, jnp.concatenate([zero, turned[:, :-1]], axis=1), turned))
        turned = pltpu.roll(values, LANES - BJ, 3)
        total = total + apply(base + 1, jnp.where(in_high, jnp.concatenate([turned[:, 1:], zero], axis=1), turned))
        total = total + apply(base + 2, jnp.where(j_first, 0.0, pltpu.roll(values, 1, 3)))
        return total + apply(base + 3, jnp.where(j_final, 0.0, pltpu.roll(values, LANES - 1, 3)))

    def scan(values, indices, reverse, length=planes):
        by = 1
        for index in indices:
            if reverse:
                shifted = jnp.where(place < length - by, pltpu.roll(values, SUBLANES - by, 2), 0.0)
            else:
                shifted = jnp.where((place >= by) & (place < length), pltpu.roll(values, by, 2), 0.0)
            values = values + apply(index, shifted)
            by *= 2
        return values

    def local(n):
        yf[...] = scan(sf[...], (FWD, F2, F4), False)
        tf[...] = cg[...] + lateral(yf[...], IM) + (yf[...] - sf[...])
        part = scan(tf[...], (BWD, B2, B4), True)
        prefix[n, sub, 0] = yf[:, :, planes - 1:planes, :]
        prefix[n, sub, 1] = part[:, :, 0:1, :]

    def send_prefix(n):
        for target in range(subs):
            @pl.when(sub != target)
            def _():
                prefix_copy(n, sub, target).start()

    def finish_prefix(n):
        for target in range(subs):
            @pl.when(sub != target)
            def _():
                prefix_copy(n, sub, target).wait_send()

    fetch[0].wait()
    starts[sub] = solution[:, :, 0:1, :]
    stage_edge(0, solution)
    pl.semaphore_wait(pltpu.get_barrier_semaphore(), count_all - 1)
    start_edge(0)
    for target in range(subs):
        @pl.when((sub > 0) & (sub != target))
        def _():
            start_copy(sub, target).start()
    fetch[2].wait()
    prepare(0, coef)
    powers(FWD, F2, F16, place + 1)
    powers(BWD, B2, B16, planes - place)
    fetch[1].wait()
    cg[...] = apply(INV, right_side[...])
    upper = jnp.where(place == planes - 1, 0.0, pltpu.roll(solution[...], planes - 1, 2))
    sf[...] = cg[...] + lateral(solution[...], IM) + apply(BWD, upper)
    local(0)
    send_prefix(0)
    combined()

    def prepare_coarse():
        for number, store in ((1, coef_one), (2, coef_two)):
            prepare(number, store)
            width = BJ >> number
            cells = rows * LANES >> (2 * number)
            inside = lane < cells
            masks = ((lane >= width) & inside, lane < cells - width,
                     ((lane & (width - 1)) != 0) & inside, ((lane & (width - 1)) != width - 1) & inside)
            for shift, mask in enumerate(masks):
                for base in (RAW + 1, IM):
                    store[base + shift] = jnp.where(mask, store[base + shift], 0.0)

    @pl.loop(0, blocks)
    def _(n):
        down[n] = found(partner, n)

    held = (found(owner_one, me), found(owner_two, me))

    for n in range(SWEEPS_FINE):
        for source in range(subs):
            @pl.when(sub != source)
            def _():
                if n == 0 and source > 0:
                    start_copy(source, sub).wait_recv()
                prefix_copy(n, source, sub).wait_recv()
        receive_edge(n)
        below = edge_w[n][source_below]
        above = edge_a[n][partner[me]]
        missing = above if n == 0 else above - old_above[...]
        ahead = jnp.where(place == subs + last, missing, 0.0)
        if n == 0:
            for s in range(last):
                ahead = jnp.where(place == subs + s, starts[s + 1], ahead)
        old_above[...] = above
        ahead = apply(BWD, ahead)
        enter = jnp.where(place == 0, below, 0.0)
        final = jnp.zeros_like(enter)
        for s in range(subs):
            if s < last:
                enter = jnp.where(place == s + 1, prefix[n, s, 0], enter)
            if s > 0:
                final = jnp.where(place == s, prefix[n, s, 1], final)
        moved = pltpu.roll(ahead, SUBLANES + 1 - subs, 2)
        enter = enter + jnp.where((place > 0) & (place < subs), moved, 0.0)
        enter = scan(enter, (F8, F16), False, subs)
        both = enter + ahead
        sides = lateral(both, G1)
        final = final + apply(G0, enter) + sides + pltpu.roll(sides, SUBLANES - subs, 2)
        final = jnp.where(place < last, pltpu.roll(final, SUBLANES - 1, 2), jnp.where(place == last, above, 0.0))
        final = scan(final, (B8, B16), True, subs)
        wide[0] = both
        wide[1] = final
        enter = wide[0, :, :, pl.ds(sub, 1), :]
        extra = jnp.where(place == planes - 1, wide[0, :, :, pl.ds(subs + sub, 1), :], 0.0)
        y = yf[...] + apply(FP, enter) + extra
        yf[...] = y
        tf[...] = cg[...] + lateral(y, IM) + (y - (sf[...] + extra))
        zf[...] = scan(tf[...], (BWD, B2, B4), True) + apply(BP, wide[1, :, :, pl.ds(sub, 1), :])
        if n + 1 < SWEEPS_FINE:
            stage_edge(n + 1, zf)
            start_edge(n + 1)
            sf[...] = cg[...] + lateral(zf[...], IM) + (zf[...] - tf[...])
            local(n + 1)
            send_prefix(n + 1)
            if n == 0:
                prepare_coarse()
                finish_edge(0)
                finish_prefix(0)
                for target in range(subs):
                    @pl.when((sub > 0) & (sub != target))
                    def _():
                        start_copy(sub, target).wait_send()

    change = zf[...] - yf[...]
    lower = jnp.where(place == 0, -wide[0, :, :, pl.ds(sub, 1), :], pltpu.roll(change, 1, 2))
    upper = jnp.where((place == planes - 1) & is_high, -old_above[...], 0.0)
    sf[...] = lateral(change, RAW + 1) + apply(RAW + 5, lower) + apply(RAW + 6, upper)

    height = rows * LANES
    r_row = lax.broadcasted_iota(jnp.int32, (height, LANES), 0)
    r_col = lax.broadcasted_iota(jnp.int32, (height, LANES), 1)
    half = BJ // 2
    share = ((((r_row >> 5) * half) + ((r_row & (BJ - 1)) >> 1)) == r_col).astype(jnp.float32)
    reduced = None
    for r in range(rows):
        both = jnp.concatenate([sf[:, r].reshape(NV * SUBLANES, LANES), zf[:, r].reshape(NV * SUBLANES, LANES)], axis=0)
        term = chosen(both, share[r * LANES:(r + 1) * LANES])
        reduced = term if reduced is None else reduced + term
    count = NV * planes // 2
    rsum[...] = reduced * 0.125
    gathered[sub, me, 0:count, :] = rsum[pl.ds(0, count, stride=2), :] + rsum[pl.ds(1, count, stride=2), :]
    gathered[sub, me, count:count + NV, :] = rsum[pl.ds(NV * planes + planes - 1, NV, stride=planes), :]
    gathered[sub, me, count + NV:count + 2 * NV, :] = rsum[pl.ds(NV * planes, NV, stride=planes), :]

    def spread_copy(source, target):
        return pltpu.make_async_remote_copy(
            src_ref=gathered.at[sub, source], dst_ref=gathered.at[sub, source], send_sem=gs_sem.at[target],
            recv_sem=gr_sem.at[source], device_id=(target, sub), device_id_type=MESH)

    @pl.loop(1, blocks)
    def _(step):
        spread_copy(me, peer(step)).start()

    def across_copy(source, block, target):
        return pltpu.make_async_remote_copy(
            src_ref=gathered.at[source, block], dst_ref=gathered.at[source, block],
            send_sem=es_sem.at[target, block], recv_sem=er_sem.at[source, block],
            device_id=(me, target), device_id_type=MESH)

    for step in range(1, subs):
        across_copy(sub, me, after(sub, step, subs)).start()

    stage_edge(SWEEPS_FINE, zf)
    start_edge(SWEEPS_FINE)
    low_recv[0] = zf[:, :, planes - 1:planes, :]

    def halo_copy(target):
        return pltpu.make_async_remote_copy(
            src_ref=low_recv.at[0], dst_ref=low_recv.at[1], send_sem=hs_sem.at[0], recv_sem=hr_sem.at[0],
            device_id=(me, target), device_id_type=MESH)

    @pl.when(jnp.logical_not(is_high))
    def _():
        halo_copy(sub + 1).start()

    @pl.loop(1, blocks)
    def _(step):
        source = after(me, step, blocks)
        spread_copy(source, source).wait_recv()
        for turn in range(1, subs):
            across_copy(sub, source, after(sub, turn, subs)).start()

    for n in range(1, SWEEPS_FINE):
        finish_edge(n)
        finish_prefix(n)

    @pl.loop(1, blocks)
    def _(step):
        spread_copy(me, after(me, step, blocks)).wait_send()

    receive_edge(SWEEPS_FINE)

    @pl.when(is_low)
    def _():
        low_recv[1] = edge_w[SWEEPS_FINE][source_below]

    @pl.when(is_high)
    def _():
        fresh = apply(RAW + 6, edge_a[SWEEPS_FINE][partner[me]], 1)
        sf[:, :, planes - 1:planes, :] = sf[:, :, planes - 1:planes, :] + fresh

    @pl.when(jnp.logical_not(is_low))
    def _():
        halo_copy(sub).wait_recv()

    sf[:, :, 0:1, :] = sf[:, :, 0:1, :] + apply(RAW + 5, low_recv[1], 1)
    residual = sf[...]
    squares_recv[me] = jnp.sum((residual * residual).reshape(NV * rows * SUBLANES, LANES), axis=0, keepdims=True)

    def norm_copy(source, target):
        return pltpu.make_async_remote_copy(
            src_ref=squares_recv.at[source], dst_ref=squares_recv.at[source], send_sem=ns_sem.at[target],
            recv_sem=nr_sem.at[source], device_id=(target, sub), device_id_type=MESH)

    def total_copy(source, target):
        return pltpu.make_async_remote_copy(
            src_ref=totals.at[source], dst_ref=totals.at[source], send_sem=ts_sem.at[target],
            recv_sem=tr_sem.at[source], device_id=(me, target), device_id_type=MESH)

    @pl.loop(1, blocks)
    def _(step):
        norm_copy(me, peer(step)).start()

    @pl.loop(0, blocks)
    def _(block):
        for turn in range(1, subs):
            source = after(sub, turn, subs)
            across_copy(source, block, source).wait_recv()

    def use(store, index, values):
        cut = values.reshape(NV, -1, SUBLANES, LANES)
        terms = [store[index, b][:, None] * cut[b][None] for b in range(NV)]
        out = (terms[0] + terms[1]) + (terms[2] + terms[3]) + terms[4]
        return out.reshape(values.shape)

    slot = lax.broadcasted_iota(jnp.int32, (blocks, 1), 0)

    def codes(source):
        out = jnp.zeros((blocks, 1), jnp.int32)
        for n in range(blocks):
            out = jnp.where(slot == n, source(n), out)
        return out

    code_below = codes(lambda n: orient[down[n]])
    code_above = codes(lambda n: orient[n])

    def turned(values, code, cells, width):
        high = jnp.where((code & 1) != 0, cells - width, 0)
        return permute(values, lane ^ high ^ jnp.where(code >= 2, width - 1, 0))

    local_planes = planes // 2
    cells_one = rows * LANES // 4

    def edge_rows(s, pick, first):
        return jnp.stack([
            jnp.concatenate([gathered[s, pl.ds(pick(n), 1), first + a, :] for n in range(blocks)], axis=0)
            for a in range(NV)])

    under = turned(edge_rows(last, lambda n: down[n], count), code_below, cells_one, BJ // 2)
    over = turned(edge_rows(0, lambda n: partner[n], count + NV), code_above, cells_one, BJ // 2)
    for s in range(subs):
        if s > 0:
            under = jnp.stack([gathered[s - 1, :, count + a, :] for a in range(NV)])
        under = use(coef, RAW + 5, under)
        for k in range(local_planes):
            value = jnp.stack([gathered[s, :, a * local_planes + k, :] for a in range(NV)])
            if k == 0:
                value = value + under
            if s == last and k == local_planes - 1:
                value = value + use(coef, RAW + 6, over)
            field_f[:, s * local_planes + k] = value

    def root_mean(value, entries):
        return jnp.sqrt(jnp.sum(value, axis=1, keepdims=True) / jnp.float32(entries))

    size = NV * blocks * subs * planes * rows * LANES

    def level(store, cells, width, g, c, p, v, y, sweeps):
        depth = g.shape[1]
        chunk = max(1, 2 * SUBLANES // blocks)
        steps = depth // chunk

        def repeat(body, start, number):
            return lax.fori_loop(0, number, body, start, unroll=blocks <= SUBLANES)

        def sides(values, base):
            axis = values.ndim - 1
            out = use(store, base, pltpu.roll(values, width, axis))
            out = out + use(store, base + 1, pltpu.roll(values, LANES - width, axis))
            out = out + use(store, base + 2, pltpu.roll(values, 1, axis))
            return out + use(store, base + 3, pltpu.roll(values, LANES - 1, axis))

        def interfaces():
            below = jnp.concatenate([v[:, depth - 1, pl.ds(down[n], 1), :] for n in range(blocks)], axis=1)
            above = jnp.concatenate([v[:, 0, pl.ds(partner[n], 1), :] for n in range(blocks)], axis=1)
            return turned(below, code_below, cells, width), turned(above, code_above, cells, width)

        def centre(step, carry):
            at = pl.ds(step * chunk, chunk)
            c[:, at] = use(store, INV, g[:, at])
            return carry

        repeat(centre, 0, steps)
        nothing = jnp.zeros((NV, blocks, LANES), jnp.float32)
        below, above = nothing, nothing
        for n in range(sweeps):
            if n > 0:
                below, above = interfaces()
                p[:, depth - 1] = use(store, BWD, above)

            def forward(step, previous):
                at = pl.ds(step * chunk, chunk)
                s = c[:, at]
                if n > 0:
                    s = s + sides(v[:, at], IM) + p[:, at]
                made = []
                for u in range(chunk):
                    behind = use(store, FWD, previous)
                    previous = s[:, u] + behind
                    made.append((previous, behind))
                for u, (now, behind) in enumerate(made):
                    y[:, step * chunk + u] = now
                    p[:, step * chunk + u] = behind
                return previous

            repeat(forward, below, steps)

            def backward(step, following):
                start = depth - chunk - step * chunk
                at = pl.ds(start, chunk)
                t = c[:, at] + sides(y[:, at], IM) + p[:, at]
                made = []
                for u in range(chunk - 1, -1, -1):
                    ahead = use(store, BWD, following)
                    following = t[:, u] + ahead
                    made.append((u, following, ahead))
                for u, now, ahead in made:
                    v[:, start + u] = now
                    p[:, start + u] = ahead
                return following

            repeat(backward, above, steps)

        new_below, new_above = interfaces()
        top = use(store, RAW + 6, new_above - above)

        def remain(step, carry, final=False):
            squares, previous = carry
            at = pl.ds(step * chunk, chunk)
            change = v[:, at] - y[:, at]
            shifted = jnp.stack([previous] + [change[:, u] for u in range(chunk - 1)], axis=1)
            out = sides(change, RAW + 1) + use(store, RAW + 5, shifted)
            if final:
                out = jnp.stack([out[:, u] for u in range(chunk - 1)] + [out[:, chunk - 1] + top], axis=1)
            c[:, at] = out
            return squares + jnp.sum(out * out, axis=1), change[:, chunk - 1]

        carry = repeat(remain, (nothing, new_below - below), steps - 1)
        squares, _ = remain(steps - 1, carry, True)
        return jnp.sum(squares.reshape(NV * blocks, LANES), axis=0, keepdims=True)

    depth_one = field_f.shape[1]
    total = level(coef_one, cells_one, BJ // 2, field_f, field_c, field_p, field_v, field_y, SWEEPS_MID)
    norms[1:2, :] = jnp.broadcast_to(root_mean(total, size // 8), (1, LANES))

    @pl.loop(1, blocks)
    def _(step):
        source = peer(step)
        norm_copy(source, source).wait_recv()

    totals[sub] = jnp.sum(squares_recv[...].reshape(blocks, LANES), axis=0, keepdims=True)
    for turn in range(1, subs):
        total_copy(sub, after(sub, turn, subs)).start()

    @pl.loop(1, blocks)
    def _(step):
        norm_copy(me, peer(step)).wait_send()

    s_row = lax.broadcasted_iota(jnp.int32, (LANES, LANES), 0)
    s_col = lax.broadcasted_iota(jnp.int32, (LANES, LANES), 1)
    fold = ((((s_row >> 4) * (BJ // 4)) + ((s_row & (BJ // 2 - 1)) >> 1)) == s_col).astype(jnp.float32)
    depth_two = depth_one // 2

    pairs = jnp.stack([field_c[:, 2 * k] + field_c[:, 2 * k + 1] for k in range(depth_two)], axis=1)
    two_f[...] = chosen(pairs.reshape(-1, LANES) * 0.125, fold).reshape(two_f.shape)

    total = level(coef_two, cells_one // 4, BJ // 4, two_f, two_c, two_p, two_v, two_y, SWEEPS_COARSE)
    norms[2:3, :] = jnp.broadcast_to(root_mean(total, size // 64), (1, LANES))

    unfold = ((((s_col >> 4) * (BJ // 4)) + ((s_col & (BJ // 2 - 1)) >> 1)) == s_row).astype(jnp.float32)
    coarse_planes = local_planes // 2
    for which, block in enumerate((me, held[0])):
        for a in range(NV):
            for k in range(coarse_planes):
                row = (which * NV + a) * coarse_planes + k
                rsum[row:row + 1, :] = two_v[a, sub * coarse_planes + k, pl.ds(block, 1), :]
    for a in range(NV):
        for k in range(coarse_planes):
            out_two[a, pl.ds(k, 1), :] = two_v[a, sub * coarse_planes + k, pl.ds(held[1], 1), :]
    filled = -(-2 * NV * coarse_planes // SUBLANES) * SUBLANES
    rsum[0:filled, :] = chosen(rsum[0:filled, :], unfold)
    for a in range(NV):
        for k in range(local_planes):
            at = sub * local_planes + k
            mine = a * coarse_planes + k // 2
            row = field_v[a, at, pl.ds(me, 1), :] + rsum[mine:mine + 1, :]
            spread[pl.ds(a * planes + 2 * k, 2), :] = jnp.broadcast_to(row, (2, LANES))
            mine = mine + NV * coarse_planes
            out_one[a, pl.ds(k, 1), :] = field_v[a, at, pl.ds(held[0], 1), :] + rsum[mine:mine + 1, :]

    for r in range(rows):
        grow = ((((s_col + r * LANES) >> 5) * half) + ((s_col & (BJ - 1)) >> 1) == s_row).astype(jnp.float32)
        corrected[:, r] = zf[:, r] + chosen(spread[...], grow).reshape(NV, SUBLANES, LANES)

    @pl.loop(0, blocks)
    def _(block):
        for turn in range(1, subs):
            across_copy(sub, block, after(sub, turn, subs)).wait_send()

    finish_edge(SWEEPS_FINE)

    @pl.when(jnp.logical_not(is_high))
    def _():
        halo_copy(sub + 1).wait_send()

    for turn in range(1, subs):
        source = after(sub, turn, subs)
        total_copy(source, source).wait_recv()
    total = jnp.sum(totals[...].reshape(subs, LANES), axis=0, keepdims=True)
    norms[0:1, :] = jnp.broadcast_to(root_mean(total, size), (1, LANES))
    for turn in range(1, subs):
        total_copy(sub, after(sub, turn, subs)).wait_send()


def finish(corrected, one, two, norms, out, out_one, out_two, out_norms):
    for r in range(corrected.shape[1]):
        out[:, 0, :, r * LANES:(r + 1) * LANES] = corrected[:, r]
    out_one[:, 0] = one[...]
    out_two[:, 0] = two[:, :, :out_two.shape[3]]
    for n in range(3):
        out_norms[n] = jnp.max(norms[n:n + 1, :])


def shards(solution, right_side, couple, partner, orient, owner_one, owner_two):
    blocks = lax.axis_size("blk")
    subs = lax.axis_size("sub")
    planes, cells = solution.shape[2:]
    rows = cells // LANES
    tall = planes * subs

    def tiled(x):
        return x.reshape(NV, planes, rows, LANES).transpose(0, 2, 1, 3)

    vmem = pl.BlockSpec(memory_space=pltpu.VMEM)
    smem = pl.BlockSpec(memory_space=pltpu.SMEM)
    hbm = pl.BlockSpec(memory_space=pl.ANY)
    f32 = jnp.float32
    fine = pltpu.VMEM((NV, rows, planes, LANES), f32)
    plane = (NV, rows, 1, LANES)
    mid = pltpu.VMEM((NV, tall // 2, blocks, LANES), f32)
    low = pltpu.VMEM((NV, tall // 4, blocks, LANES), f32)
    matrix = (NV, NV, SUBLANES, LANES)
    payload = NV * planes // 2 + 2 * NV
    dma = pltpu.SemaphoreType.DMA
    edges = SWEEPS_FINE + 1
    couple = couple.transpose(2, 3, 0, 1)
    results = pl.pallas_call(
        functools.partial(kernel, (blocks, subs)),
        name="vcycle",
        out_shape=(
            pltpu.VMEM((NV, rows, planes, LANES), f32),
            pltpu.VMEM((NV, planes // 2, LANES), f32),
            pltpu.VMEM((NV, planes // 4, LANES), f32),
            pltpu.VMEM((3, LANES), f32),
        ),
        in_specs=[hbm] * 7,
        out_specs=(vmem, vmem, vmem, vmem),
        scratch_shapes=[
            pltpu.VMEM((29,) + matrix, f32), pltpu.VMEM((14,) + matrix, f32), pltpu.VMEM((14,) + matrix, f32),
            fine, fine, fine, fine, fine, pltpu.VMEM((2, NV, rows, planes, LANES), f32), pltpu.VMEM(plane, f32),
            pltpu.VMEM((edges,) + plane, f32),
            *[pltpu.VMEM((blocks,) + plane, f32)] * (2 * edges),
            pltpu.VMEM((subs,) + plane, f32),
            pltpu.VMEM((SWEEPS_FINE, subs, 2) + plane, f32),
            pltpu.VMEM((subs, blocks, payload, LANES), f32),
            pltpu.VMEM((2 * NV * planes, LANES), f32),
            pltpu.VMEM((2,) + plane, f32),
            pltpu.VMEM((blocks, 1, LANES), f32),
            pltpu.SMEM((blocks,), jnp.int32),
            mid, mid, mid, mid, mid, low, low, low, low, low,
            pltpu.VMEM((NV * planes, LANES), f32),
            dma((edges, blocks, subs)), dma((edges, blocks)), dma((edges, blocks)),
            dma((subs,)), dma((subs,)),
            dma((SWEEPS_FINE, subs)), dma((SWEEPS_FINE, subs)),
            dma((blocks,)), dma((blocks,)), dma((subs, blocks)), dma((subs, blocks)),
            dma((1,)), dma((1,)), dma((blocks,)), dma((blocks,)),
            fine, fine, pltpu.SMEM(couple.shape, f32), *[pltpu.SMEM((blocks,), jnp.int32)] * 4, dma((7,)),
            pltpu.VMEM((subs, 1, LANES), f32), dma((subs,)), dma((subs,)),
        ],
        compiler_params=pltpu.CompilerParams(collective_id=0, has_side_effects=True, vmem_limit_bytes=60 * 1024 * 1024),
    )(tiled(solution), tiled(right_side), couple, partner, orient, owner_one, owner_two)
    return pl.pallas_call(
        finish,
        name="finish",
        out_shape=(
            jax.ShapeDtypeStruct((NV, 1, planes, cells), f32),
            jax.ShapeDtypeStruct((NV, 1, planes // 2, cells // 4), f32),
            jax.ShapeDtypeStruct((NV, 1, planes // 4, cells // 16), f32),
            jax.ShapeDtypeStruct((3,), f32),
        ),
        in_specs=[vmem] * 4,
        out_specs=(vmem, vmem, vmem, smem),
    )(*[pltpu.with_memory_space_constraint(x, pltpu.VMEM) for x in results])


def solution(mesh):
    split = P(None, "blk", "sub", None)
    return jax.shard_map(
        shards,
        mesh=mesh,
        in_specs=(split, split, P(), P(), P(), P(), P()),
        out_specs=(split, split, split, P()),
        check_vma=False,
    )
```
